256 devices in a mesh: row: 8 (over x, core), col: 4 (over y), depth: 8 (over z).
Axes of the slice: x: 4, y: 4, z: 8, core: 2. Of those that a mesh axis runs over, the one named last changes fastest.
Arguments:
- left_values: bfloat16 [384, 32, 4, 529], P('row', ('col', 'depth')), may hold values from -1.25 to 1.25
- left_columns: int32 [384, 32, 4], P('row', ('col', 'depth')), may hold values from 0 to 39, as said below
- right_values: bfloat16 [32, 40, 4, 3, 529], P(('col', 'depth'), 'row'), may hold values from -1.75 to 1.75
- right_columns: int32 [32, 40, 4, 3], P(('col', 'depth'), 'row'), may hold values from 0 to 31, as said below
Outputs:
- product_matrix: bfloat16 [8832, 2944], P('row', ('col', 'depth'))
The draws below stay inside these ranges and needn't reach their ends.
Inputs may be any that keep to these rules, and one draw needn't show every extreme that they name: `left_columns`: within one block row and panel the 4 entries are distinct. `right_columns`: within one block row and column tile the 3 entries are distinct.
All inputs are finite; a program needn't handle non-finite values.
Results may differ from the reference program's by a relative error of at most 0.001.
Values may be sent and summed in bfloat16 or wider, within the bound.
No kernel may reach another device: no remote copies, remote signals or barrier semaphores. Data moves between devices by JAX's collectives and lax.ppermute only.
A program may use at most 128 MiB of HBM per device.

```python
import jax
import jax.numpy as jnp
from jax import lax

BLK = 23
PANEL = 40
KPAN = 32
SAP = 4
CT = 4
CTW = 32
SBP = 3
MB = 384
NB = 128


def distinct_columns(key, leading, choices, count):
    scores = jax.random.randint(key, leading + (choices,), 0, 1 << 20) * choices + jnp.arange(choices, dtype=jnp.int32)
    chosen = lax.top_k(scores, count)[1]
    return chosen.astype(jnp.int32)


def draw_left_columns(key, part):
    return distinct_columns(jax.random.fold_in(key, 11), (MB, KPAN), PANEL, SAP)


def draw_right_columns(key, part):
    return distinct_columns(jax.random.fold_in(key, 12), (KPAN, PANEL, CT), CTW, SBP)


def level_of(own_key, shape, pieces, smallest, high):
    factor_of, own = 1.0, jax.random.fold_in(own_key, 6)
    for dim, blocks in pieces:
        draws = jnp.exp(jax.random.uniform(jax.random.fold_in(own, dim), (blocks,), jnp.float32, smallest / len(pieces), high / len(pieces)))
        factor_of = factor_of * jnp.repeat(draws, shape[dim] // blocks).reshape([-1 if axis == dim else 1 for axis in range(len(shape))])
    return factor_of


def centred(rng, shape, width, most, pieces=(), held_as=jnp.bfloat16):
    loudness = level_of(rng, shape, pieces, -0.22, 0.18) if pieces else 1.0
    result = jax.random.normal(rng, shape, jnp.float32) * width * loudness
    return jnp.minimum(jnp.maximum(result, -most), most).astype(held_as)


def setup_inputs(seed: int = 0) -> dict:
    key_list = jax.random.split(jax.random.key(seed), 5)
    return {
        "left_values": centred(key_list[0], (MB, KPAN, SAP, BLK * BLK), BLK ** -0.5, 1.25, ((0, 8), (1, 32))),
        "left_columns": draw_left_columns(jax.random.fold_in(key_list[4], 71), 0),
        "right_values": centred(key_list[2], (KPAN, PANEL, CT, SBP, BLK * BLK), (SAP * SBP * KPAN // CTW) ** -0.5, 1.75, ((0, 32), (1, 8))),
        "right_columns": draw_right_columns(jax.random.fold_in(key_list[4], 71), 0),
    }


def reference(left_values, left_columns, right_values, right_columns):
    tile_base = (jnp.arange(CT, dtype=jnp.int32) * CTW)[None, None, :, None]
    row_ids = jnp.broadcast_to(jnp.arange(MB, dtype=jnp.int32)[:, None], (MB, SAP * CT * SBP))

    def panel_step(running, items):
        left_panel, left_cols, right_panel, right_cols = items
        chosen = right_panel[left_cols]
        chosen_cols = right_cols[left_cols] + tile_base
        left_mats = left_panel.astype(jnp.float32).reshape(MB, SAP, BLK, BLK)
        right_mats = chosen.astype(jnp.float32).reshape(MB, SAP, CT * SBP, BLK, BLK)
        partial_blocks = jnp.einsum("isab,isnbc->isnac", left_mats, right_mats, precision=lax.Precision.HIGHEST)
        partial_blocks = partial_blocks.reshape(MB, SAP * CT * SBP, BLK * BLK)
        running = running.at[row_ids, chosen_cols.reshape(MB, SAP * CT * SBP)].add(partial_blocks)
        return running, None

    start_blocks = jnp.zeros((MB, NB, BLK * BLK), jnp.float32)
    items = (jnp.transpose(left_values, (1, 0, 2, 3)), jnp.transpose(left_columns, (1, 0, 2)), right_values, right_columns)
    summed, unused = lax.scan(panel_step, start_blocks, items)
    dense = jnp.transpose(summed.reshape(MB, NB, BLK, BLK), (0, 2, 1, 3)).reshape(MB * BLK, NB * BLK)
    return dense.astype(jnp.bfloat16)
```

```python
import functools

import jax
import jax.numpy as jnp
from jax import lax
from jax.experimental import pallas as pl
from jax.experimental.pallas import tpu as pltpu
from jax.sharding import PartitionSpec as P

BLK = 23
LANES = 128
APAD = 24
KROW = 32
SLOTS = 4
USLOTS = 3
TILES = 4
PANEL = 40
HERE = 5
GROUP = 8
CHUNK = 96
WIDE = 4 * CHUNK
ROWS = 48


def place(z, windows, lane, src, dst):
    first, last = src // LANES, (src + BLK - 1) // LANES
    shift = (dst - src) % LANES
    split = dst + min(BLK, LANES * (first + 1) - src)
    rolled = pltpu.roll(windows(first), shift, 1) if shift else windows(first)
    z = jnp.where((lane >= dst) & (lane < split), rolled, z)
    if last != first:
        rolled = pltpu.roll(windows(last), shift, 1) if shift else windows(last)
        z = jnp.where((lane >= split) & (lane < dst + BLK), rolled, z)
    return z


def pack_kernel(left_ref, left_cols_ref, right_ref, right_cols_ref, left_out, right_out, left_tmp, right_tmp):
    lane = lax.broadcasted_iota(jnp.int32, (ROWS, LANES), 1)
    for a in range(BLK):
        z = jnp.zeros((ROWS, LANES), jnp.float32)
        for s in range(SLOTS):
            z = place(
                z,
                lambda j, s=s: left_ref[s, :, j * LANES : (j + 1) * LANES],
                lane,
                BLK * a,
                KROW * s,
            )
        left_tmp[pl.ds(a, ROWS, stride=APAD), :] = z
    left_tmp[pl.ds(BLK, ROWS, stride=APAD), :] = left_cols_ref[...]
    for i in range(ROWS):
        left_out[i] = left_tmp[i * APAD : (i + 1) * APAD, :].astype(jnp.bfloat16)
    lane = lax.broadcasted_iota(jnp.int32, (16, LANES), 1)
    for a in range(BLK):
        z = jnp.zeros((16, LANES), jnp.float32)
        for k in range(HERE):
            z = place(
                z,
                lambda j, k=k: right_ref[k, :, j * LANES : (j + 1) * LANES],
                lane,
                BLK * a,
                BLK * k,
            )
        right_tmp[pl.ds(a, 16, stride=APAD), :] = z
    right_tmp[pl.ds(BLK, 16, stride=APAD), :] = right_cols_ref[...]
    for d in range(GROUP):
        for u in range(USLOTS):
            row = (d // 2) * 4 + u
            right_out[d, u] = right_tmp[row * APAD : (row + 1) * APAD, :].astype(jnp.bfloat16)


def pack(left_values, left_columns, right_values, right_columns):
    wide = 5 * LANES
    left = jnp.pad(
        jnp.transpose(left_values[:, 0].astype(jnp.float32), (1, 0, 2)), ((0, 0), (0, 0), (0, wide - BLK * BLK))
    )
    left_cols = jnp.pad(left_columns[:, 0].astype(jnp.float32), ((0, 0), (0, LANES - SLOTS)))
    right = jnp.pad(
        right_values[0].astype(jnp.float32), ((0, 0), (0, 0), (0, 1), (0, wide - BLK * BLK))
    ).reshape(HERE, 16, wide)
    right_cols = jnp.pad(
        jnp.transpose(right_columns[0], (1, 2, 0)).astype(jnp.float32), ((0, 0), (0, 1), (0, LANES - HERE))
    ).reshape(16, LANES)
    return pl.pallas_call(
        pack_kernel,
        out_shape=(
            jax.ShapeDtypeStruct((ROWS, APAD, LANES), jnp.bfloat16),
            jax.ShapeDtypeStruct((GROUP, USLOTS, APAD, LANES), jnp.bfloat16),
        ),
        in_specs=[pl.BlockSpec(memory_space=pltpu.VMEM)] * 4,
        out_specs=(pl.BlockSpec(memory_space=pltpu.VMEM),) * 2,
        scratch_shapes=[
            pltpu.VMEM((ROWS * APAD, LANES), jnp.float32),
            pltpu.VMEM((16 * APAD, LANES), jnp.float32),
        ],
    )(left, left_cols, right, right_cols)


def product_kernel(lidx_ref, dest_ref, right_ref, *refs):
    lefts, (out_ref, wide_ref, sum_ref, part_ref) = refs[:GROUP], refs[GROUP:]
    lane = lax.broadcasted_iota(jnp.int32, (APAD, WIDE), 1)

    def fill(n, carry):
        for k in range(HERE):
            z = jnp.zeros((APAD, WIDE), jnp.float32)
            for u in range(USLOTS):
                at = dest_ref[(n * USLOTS + u) * HERE + k]
                block = right_ref[n, u].astype(jnp.float32)
                rolled = pltpu.roll(block, (at + 4 * LANES - BLK * k) % LANES, 1)
                rolled = jnp.concatenate([rolled] * 3, axis=1)
                z = jnp.where((lane >= at) & (lane < at + BLK), rolled, z)
            full = jnp.concatenate([z, jnp.zeros((KROW - APAD, WIDE), jnp.float32)], axis=0)
            full = full.astype(jnp.bfloat16)
            for q in range(3):
                wide_ref[n * HERE + k, q] = full[:, q * LANES : (q + 1) * LANES]
        return carry

    lax.fori_loop(0, 8 * GROUP, fill, 0)

    def step(g, carry):
        for m in range(8):
            i = g * 8 + m
            total = jnp.zeros((APAD, WIDE), jnp.float32)
            for j in range(0, GROUP, 2):
                at = [lidx_ref[(i * GROUP + j) * SLOTS + s] for s in range(2 * SLOTS)]
                weights = jnp.concatenate(
                    [jnp.concatenate([wide_ref[n, q] for n in at], axis=0) for q in range(3)], axis=1
                )
                rows = jnp.concatenate([lefts[j][i], lefts[j + 1][i]], axis=1)
                total = total + jnp.dot(rows, weights, preferred_element_type=jnp.float32)
            part_ref[m * BLK : m * BLK + APAD, :] = total
        sum_ref[pl.ds(pl.multiple_of(g * 8 * BLK, 8), 8 * BLK), :] = part_ref[0 : 8 * BLK, :]
        return carry

    lax.fori_loop(0, ROWS // 8, step, 0)
    count = ROWS * BLK
    for q in range(3):
        turned = sum_ref[0:1152, q * LANES : (q + 1) * LANES].T
        out_ref[q * LANES : (q + 1) * LANES, :] = turned[:, :count]


def product(lidx, dest, right, lefts):
    return pl.pallas_call(
        product_kernel,
        out_shape=jax.ShapeDtypeStruct((WIDE, ROWS * BLK), jnp.float32),
        in_specs=[pl.BlockSpec(memory_space=pltpu.SMEM)] * 2
        + [pl.BlockSpec(memory_space=pltpu.VMEM)] * (1 + GROUP),
        out_specs=pl.BlockSpec(memory_space=pltpu.VMEM),
        scratch_shapes=[
            pltpu.VMEM((GROUP * PANEL, 3, KROW, LANES), jnp.bfloat16),
            pltpu.VMEM((1152, WIDE), jnp.float32),
            pltpu.VMEM((8 * APAD, WIDE), jnp.float32),
        ],
        cost_estimate=pl.CostEstimate(flops=6_000_000_000, bytes_accessed=8_000_000, transcendentals=0),
    )(lidx, dest, right, *lefts)


def shift(x, axis, by, n):
    return lax.ppermute(x, axis, [(i, (i + by) % n) for i in range(n)])


def gather_depth(own):
    f1, b1 = shift(own, "depth", 1, 8), shift(own, "depth", -1, 8)
    f2, b2 = shift(f1, "depth", 1, 8), shift(b1, "depth", -1, 8)
    f3, b3 = shift(f2, "depth", 1, 8), shift(b2, "depth", -1, 8)
    half = ROWS // 2
    f4, b4 = shift(f3[:half], "depth", 1, 8), shift(b3[half:], "depth", -1, 8)
    far = jnp.concatenate([f4, b4], axis=0)
    return [own, f1, b1, f2, b2, f3, b3, far], (0, -1, 1, -2, 2, -3, 3, 4)


def body(left_values, left_columns, right_values, right_columns):
    c, d = lax.axis_index("col"), lax.axis_index("depth")
    left, right = pack(left_values, left_columns, right_values, right_columns)
    lefts, offsets = gather_depth(left)
    right = lax.all_to_all(right, "depth", 0, 0)
    first = lax.all_gather(right[:4], "row", axis=1)
    second = lax.all_gather(right[4:], "row", axis=1)
    right = jnp.concatenate([first, second], axis=0).reshape(64, USLOTS, APAD, LANES)
    rcol = right[:, :, BLK, :HERE].astype(jnp.int32)
    local = rcol - 16 * (d % 2)
    dest = jnp.where(
        (local >= 0) & (local < 16), CHUNK * ((local // 4 - c) % 4) + BLK * (local % 4), 4 * LANES
    )
    lidx = jnp.stack(
        [x[:, BLK, :SLOTS].astype(jnp.int32) + PANEL * ((d + o) % 8) for x, o in zip(lefts, offsets)], axis=1
    )
    parts = product(lidx.reshape(-1), dest.reshape(-1), right, lefts)
    own, ahead, far, behind = (parts[CHUNK * q : CHUNK * q + 4 * BLK] for q in range(4))
    cut = 48
    from_behind = shift(far[:cut], "col", 1, 4)
    from_ahead = shift(far[cut:], "col", -1, 4)
    ahead = jnp.concatenate([ahead[:cut] + from_behind, ahead[cut:]], axis=0)
    behind = jnp.concatenate([behind[:cut], behind[cut:] + from_ahead], axis=0)
    total = own + shift(ahead, "col", 1, 4) + shift(behind, "col", -1, 4)
    done = total.astype(jnp.bfloat16)
    home = [(y * 8 + z, (z // 2) * 8 + (z % 2) * 4 + y) for y in range(4) for z in range(8)]
    return lax.ppermute(done, ("col", "depth"), home).T


def solution(mesh):
    placed = (
        P("row", ("col", "depth"), None, None),
        P("row", ("col", "depth"), None),
        P(("col", "depth"), "row", None, None, None),
        P(("col", "depth"), "row", None, None),
    )
    return jax.shard_map(
        body, mesh=mesh, in_specs=placed, out_specs=P("row", ("col", "depth")), check_vma=False
    )
```

```python
import jax
import jax.numpy as jnp
from jax import lax
from jax.experimental import pallas as pl
from jax.experimental.pallas import tpu as pltpu
from jax.sharding import PartitionSpec as P


BLK = 23
LANES = 128
APAD = 24
KROW = 32
SLOTS = 4
USLOTS = 3
PANEL = 40
HERE = 5
GROUP = 8
CHUNK = 96
WIDE = 4 * CHUNK
ROWS = 48
OFFSETS = (0, 7, 1, 6, 2, 5, 3, 4)


def place(z, windows, lane, src, dst):
    first, last = src // LANES, (src + BLK - 1) // LANES
    shift = (dst - src) % LANES
    split = dst + min(BLK, LANES * (first + 1) - src)
    rolled = pltpu.roll(windows(first), shift, 1) if shift else windows(first)
    z = jnp.where((lane >= dst) & (lane < split), rolled, z)
    if last != first:
        rolled = pltpu.roll(windows(last), shift, 1) if shift else windows(last)
        z = jnp.where((lane >= split) & (lane < dst + BLK), rolled, z)
    return z


def pack_kernel(left_ref, right_ref, right_cols_ref, left_out, right_out, left_tmp, right_tmp):
    lane = lax.broadcasted_iota(jnp.int32, (ROWS, LANES), 1)
    for a in range(BLK):
        z = jnp.zeros((ROWS, LANES), jnp.float32)
        for s in range(SLOTS):
            z = place(
                z,
                lambda j, s=s: left_ref[s, :, j * LANES : (j + 1) * LANES],
                lane,
                BLK * a,
                KROW * s,
            )
        left_tmp[pl.ds(a, ROWS, stride=APAD), :] = z
    left_tmp[pl.ds(BLK, ROWS, stride=APAD), :] = jnp.zeros((ROWS, LANES), jnp.float32)
    for i in range(ROWS):
        left_out[i] = left_tmp[i * APAD : (i + 1) * APAD, :].astype(jnp.bfloat16)
    lane = lax.broadcasted_iota(jnp.int32, (16, LANES), 1)
    for a in range(BLK):
        z = jnp.zeros((16, LANES), jnp.float32)
        for k in range(HERE):
            z = place(
                z,
                lambda j, k=k: right_ref[k, :, j * LANES : (j + 1) * LANES],
                lane,
                BLK * a,
                BLK * k,
            )
        right_tmp[pl.ds(a, 16, stride=APAD), :] = z
    right_tmp[pl.ds(BLK, 16, stride=APAD), :] = right_cols_ref[...]
    for d in range(GROUP):
        for u in range(USLOTS):
            row = (d % 4) * 4 + u
            right_out[d, u] = right_tmp[row * APAD : (row + 1) * APAD, :].astype(jnp.bfloat16)


def pack(left_values, left_columns, right_values, right_columns):
    wide = 5 * LANES
    left = jnp.pad(
        jnp.transpose(left_values[:, 0].astype(jnp.float32), (1, 0, 2)), ((0, 0), (0, 0), (0, wide - BLK * BLK))
    )
    right = jnp.pad(
        right_values[0].astype(jnp.float32), ((0, 0), (0, 0), (0, 1), (0, wide - BLK * BLK))
    ).reshape(HERE, 16, wide)
    left_cols = jnp.pad(left_columns[:, 0].astype(jnp.float32).reshape(2, 96), ((0, 2), (16, 16)))
    right_cols = jnp.pad(
        jnp.transpose(right_columns[0], (1, 2, 0)).astype(jnp.float32), ((0, 0), (0, 1), (0, LANES - HERE))
    )
    right_cols = (right_cols + left_cols[None]).reshape(16, LANES)
    return pl.pallas_call(
        pack_kernel,
        out_shape=(
            jax.ShapeDtypeStruct((ROWS, APAD, LANES), jnp.bfloat16),
            jax.ShapeDtypeStruct((GROUP, USLOTS, APAD, LANES), jnp.bfloat16),
        ),
        in_specs=[pl.BlockSpec(memory_space=pltpu.VMEM)] * 3,
        out_specs=(pl.BlockSpec(memory_space=pltpu.VMEM),) * 2,
        scratch_shapes=[
            pltpu.VMEM((ROWS * APAD, LANES), jnp.float32),
            pltpu.VMEM((16 * APAD, LANES), jnp.float32),
        ],
    )(left, right, right_cols)


def product_kernel(meta_ref, lcol_ref, dest_ref, right_ref, *refs):
    lefts, (out_ref, wide_ref, sum_ref, part_ref) = refs[:GROUP], refs[GROUP:]
    lane = lax.broadcasted_iota(jnp.int32, (APAD, WIDE), 1)

    depth, core = meta_ref[0], meta_ref[1]
    panels = [(depth + o) % GROUP for o in OFFSETS]

    def fill(n, carry):
        row = 2 * ((n // GROUP) % 4) + lax.bitwise_xor(core, n // 32)
        base = (n % GROUP) * PANEL + row * HERE
        for k in range(HERE):
            z = jnp.zeros((APAD, WIDE), jnp.float32)
            for u in range(USLOTS):
                at = dest_ref[(n * USLOTS + u) * HERE + k]
                block = right_ref[n, u].astype(jnp.float32)
                rolled = pltpu.roll(block, (at + 4 * LANES - BLK * k) % LANES, 1)
                rolled = jnp.concatenate([rolled] * 3, axis=1)
                z = jnp.where((lane >= at) & (lane < at + BLK), rolled, z)
            full = jnp.concatenate([z, jnp.zeros((KROW - APAD, WIDE), jnp.float32)], axis=0)
            full = full.astype(jnp.bfloat16)
            for q in range(3):
                wide_ref[base + k, q] = full[:, q * LANES : (q + 1) * LANES]
        return carry

    lax.fori_loop(0, 8 * GROUP, fill, 0)

    def step(g, carry):
        for m in range(8):
            i = g * 8 + m
            total = jnp.zeros((APAD, WIDE), jnp.float32)
            for j in range(0, GROUP, 2):
                at = [
                    panels[h] * PANEL + lcol_ref[panels[h] * (ROWS * SLOTS) + i * SLOTS + s]
                    for h in (j, j + 1)
                    for s in range(SLOTS)
                ]
                weights = jnp.concatenate(
                    [jnp.concatenate([wide_ref[n, q] for n in at], axis=0) for q in range(3)], axis=1
                )
                rows = jnp.concatenate([lefts[j][i], lefts[j + 1][i]], axis=1)
                total = total + jnp.dot(rows, weights, preferred_element_type=jnp.float32)
            part_ref[m * BLK : m * BLK + APAD, :] = total
        sum_ref[pl.ds(pl.multiple_of(g * 8 * BLK, 8), 8 * BLK), :] = part_ref[0 : 8 * BLK, :]
        return carry

    lax.fori_loop(0, ROWS // 8, step, 0)
    count = ROWS * BLK
    for q in range(3):
        turned = sum_ref[0:1152, q * LANES : (q + 1) * LANES].T
        out_ref[q * LANES : (q + 1) * LANES, :] = turned[:, :count]


def product(meta, lcol, dest, right, lefts):
    return pl.pallas_call(
        product_kernel,
        out_shape=jax.ShapeDtypeStruct((WIDE, ROWS * BLK), jnp.float32),
        in_specs=[pl.BlockSpec(memory_space=pltpu.SMEM)] * 3
        + [pl.BlockSpec(memory_space=pltpu.VMEM)] * (1 + GROUP),
        out_specs=pl.BlockSpec(memory_space=pltpu.VMEM),
        scratch_shapes=[
            pltpu.VMEM((GROUP * PANEL, 3, KROW, LANES), jnp.bfloat16),
            pltpu.VMEM((1152, WIDE), jnp.float32),
            pltpu.VMEM((8 * APAD, WIDE), jnp.float32),
        ],
        cost_estimate=pl.CostEstimate(flops=6_000_000_000, bytes_accessed=8_000_000, transcendentals=0),
    )(meta, lcol, dest, right, *lefts)


def shift(x, axis, by, n):
    return lax.ppermute(x, axis, [(i, (i + by) % n) for i in range(n)])


def gather_depth(own):
    f1, b1 = shift(own, "depth", 1, 8), shift(own, "depth", -1, 8)
    f2, b2 = shift(f1, "depth", 1, 8), shift(b1, "depth", -1, 8)
    f3, b3 = shift(f2, "depth", 1, 8), shift(b2, "depth", -1, 8)
    half = ROWS // 2
    f4, b4 = shift(f3[:half], "depth", 1, 8), shift(b3[half:], "depth", -1, 8)
    far = jnp.concatenate([f4, b4], axis=0)
    return [own, f1, b1, f2, b2, f3, b3, far]


def body(left_values, left_columns, right_values, right_columns):
    c, d = lax.axis_index("col"), lax.axis_index("depth")
    left, right = pack(left_values, left_columns, right_values, right_columns)
    lefts = gather_depth(left)
    right = lax.all_to_all(right, "depth", 0, 0)
    lcol = right[:, :2, BLK, 16:112].reshape(-1).astype(jnp.int32)
    mine = lax.all_gather(right, "row", axis=0, axis_index_groups=[[0, 2, 4, 6], [1, 3, 5, 7]])
    other = lax.ppermute(mine, "row", [(i, i ^ 1) for i in range(8)])
    right = jnp.concatenate([mine, other], axis=0).reshape(64, USLOTS, APAD, LANES)
    rcol = right[:, :, BLK, :HERE].astype(jnp.int32)
    local = rcol - 16 * (d // 4)
    chunk = lax.bitwise_xor(local // 4, d % 4)
    dest = jnp.where(
        (local >= 0) & (local < 16), CHUNK * ((chunk - c) % 4) + BLK * (local % 4), 4 * LANES
    )
    meta = jnp.stack([d, lax.axis_index("row") % 2])
    parts = product(meta, lcol, dest.reshape(-1), right, lefts)
    own, ahead, far, behind = (parts[CHUNK * q : CHUNK * q + 4 * BLK] for q in range(4))
    cut = 48
    from_behind = shift(far[:cut], "col", 1, 4)
    from_ahead = shift(far[cut:], "col", -1, 4)
    ahead = jnp.concatenate([ahead[:cut] + from_behind, ahead[cut:]], axis=0)
    behind = jnp.concatenate([behind[:cut], behind[cut:] + from_ahead], axis=0)
    total = own + shift(ahead, "col", 1, 4) + shift(behind, "col", -1, 4)
    done = total.astype(jnp.bfloat16)
    home = [(y * 8 + z, (z % 4) * 8 + (z // 4) * 4 + (y ^ (z % 4))) for y in range(4) for z in range(8)]
    return lax.ppermute(done, ("col", "depth"), home).T


def solution(mesh):
    placed = (
        P("row", ("col", "depth"), None, None),
        P("row", ("col", "depth"), None),
        P(("col", "depth"), "row", None, None, None),
        P(("col", "depth"), "row", None, None),
    )
    return jax.shard_map(
        body, mesh=mesh, in_specs=placed, out_specs=P("row", ("col", "depth")), check_vma=False
    )
```

```python
import jax
import jax.numpy as jnp
from jax import lax
from jax.experimental import pallas as pl
from jax.experimental.pallas import tpu as pltpu
from jax.sharding import PartitionSpec as P


BLK = 23
LANES = 128
APAD = 24
KROW = 32
SLOTS = 4
USLOTS = 3
TILES = 4
PANEL = 40
HERE = 5
GROUP = 8
CHUNK = 96
WIDE = 4 * CHUNK
ROWS = 48
SPANS = ((0, 92), (96, 144), (144, 188), (192, 240), (240, 284), (288, 336), (336, 380))
STARTS = (0, 8, 16, 24, 28, 32, 40, 48, 56, 60)
OFFSETS = (0, 7, 1, 6, 2, 5, 3, 4)


def place(z, windows, lane, src, dst):
    first, last = src // LANES, (src + BLK - 1) // LANES
    shift = (dst - src) % LANES
    split = dst + min(BLK, LANES * (first + 1) - src)
    rolled = pltpu.roll(windows(first), shift, 1) if shift else windows(first)
    z = jnp.where((lane >= dst) & (lane < split), rolled, z)
    if last != first:
        rolled = pltpu.roll(windows(last), shift, 1) if shift else windows(last)
        z = jnp.where((lane >= split) & (lane < dst + BLK), rolled, z)
    return z


def pack_left_kernel(left_ref, out_ref, flat_ref, tmp_ref):
    for i in range(ROWS):
        block = left_ref[i].astype(jnp.float32)
        for j in range(5):
            width = min(LANES, BLK * BLK - j * LANES)
            flat_ref[j, i * SLOTS : (i + 1) * SLOTS, 0:width] = block[:, j * LANES : j * LANES + width]
    lane = lax.broadcasted_iota(jnp.int32, (ROWS, LANES), 1)
    for a in range(BLK):
        z = jnp.zeros((ROWS, LANES), jnp.float32)
        for s in range(SLOTS):
            z = place(
                z,
                lambda j, s=s: flat_ref[j, pl.ds(s, ROWS, stride=SLOTS), :],
                lane,
                BLK * a,
                KROW * s,
            )
        tmp_ref[pl.ds(a, ROWS, stride=APAD), :] = z
    tmp_ref[pl.ds(BLK, ROWS, stride=APAD), :] = jnp.zeros((ROWS, LANES), jnp.float32)
    for i in range(ROWS):
        out_ref[i] = tmp_ref[i * APAD : (i + 1) * APAD, :].astype(jnp.bfloat16)


def pack_left(left_values):
    vmem = pl.BlockSpec(memory_space=pltpu.VMEM)
    return pl.pallas_call(
        pack_left_kernel,
        out_shape=jax.ShapeDtypeStruct((ROWS, APAD, LANES), jnp.bfloat16),
        in_specs=[vmem],
        out_specs=vmem,
        scratch_shapes=[
            pltpu.VMEM((5, ROWS * SLOTS, LANES), jnp.float32),
            pltpu.VMEM((ROWS * APAD, LANES), jnp.float32),
        ],
        compiler_params=pltpu.CompilerParams(vmem_limit_bytes=8 * 1024 * 1024),
    )(left_values[:, 0])


def pack_right_kernel(meta_ref, right_ref, right_cols_ref, left_cols_ref, *refs):
    outs, (flat_ref, code_ref, tmp_ref) = refs[:TILES], refs[TILES:]
    for k in range(HERE):
        for u in range(USLOTS):
            n = (k * USLOTS + u) * 8
            flat_ref[n : n + TILES, 0 : BLK * BLK] = right_ref[k, u].astype(jnp.float32)
    code_ref[...] = jnp.zeros((8, LANES), jnp.float32)
    code_ref[0:SLOTS, 0:ROWS] = left_cols_ref[...].astype(jnp.float32)
    codes = code_ref[...]
    lane = lax.broadcasted_iota(jnp.int32, (8, LANES), 1)
    for u in range(USLOTS):
        for a in range(BLK):
            z = jnp.zeros((8, LANES), jnp.float32)
            for k in range(HERE):
                n = (k * USLOTS + u) * 8
                z = place(
                    z,
                    lambda j, n=n: flat_ref[n : n + 8, j * LANES : (j + 1) * LANES],
                    lane,
                    BLK * a,
                    BLK * k,
                )
            tmp_ref[u, pl.ds(a, 8, stride=APAD), :] = z
        code_ref[...] = jnp.zeros((8, LANES), jnp.float32)
        code_ref[0:TILES, 0:HERE] = right_cols_ref[u].astype(jnp.float32)
        z = code_ref[...]
        if u < 2:
            for h in range(2):
                line = codes[2 * u + h : 2 * u + h + 1, :]
                z = z + pltpu.roll(jnp.broadcast_to(line, (8, LANES)), 16 + ROWS * h, 1)
        tmp_ref[u, pl.ds(BLK, 8, stride=APAD), :] = z
    for t in range(TILES):
        tile = (meta_ref[0] + t) % TILES
        for u in range(USLOTS):
            rows = tmp_ref[u, pl.ds(pl.multiple_of(tile * APAD, 8), APAD), :]
            outs[t][u] = rows.astype(jnp.bfloat16)


def pack_right(meta, right_values, right_columns, left_columns):
    vmem = pl.BlockSpec(memory_space=pltpu.VMEM)
    return pl.pallas_call(
        pack_right_kernel,
        out_shape=(jax.ShapeDtypeStruct((USLOTS, APAD, LANES), jnp.bfloat16),) * TILES,
        in_specs=[pl.BlockSpec(memory_space=pltpu.SMEM)] + [vmem] * 3,
        out_specs=(vmem,) * TILES,
        scratch_shapes=[
            pltpu.VMEM((HERE * USLOTS * 8, 5 * LANES), jnp.float32),
            pltpu.VMEM((8, LANES), jnp.float32),
            pltpu.VMEM((USLOTS, 8 * APAD, LANES), jnp.float32),
        ],
        compiler_params=pltpu.CompilerParams(vmem_limit_bytes=8 * 1024 * 1024),
    )(
        meta,
        jnp.transpose(right_values[0], (0, 2, 1, 3)),
        jnp.transpose(right_columns[0], (2, 1, 0)),
        jnp.transpose(left_columns[:, 0], (1, 0)),
    )


def fill_kernel(meta_ref, *refs):
    rights, (wide_ref, table_ref) = refs[:-6], refs[-6:-4]
    right_ref, mixed_ref, codes_ref, sem = refs[-4:]
    depth, core, side, col = (meta_ref[m] for m in range(4))
    for source, piece in enumerate(rights):
        count = 1 if len(piece.shape) == 3 else piece.shape[0]
        start = STARTS[source]
        block = piece[...].reshape(count, USLOTS, APAD, LANES)
        right_ref[start : start + count] = block
        codes = block[:, :, BLK, :].astype(jnp.float32).astype(jnp.int32)
        local = codes - 16 * (depth // 4)
        chunk = lax.bitwise_xor(lax.shift_right_arithmetic(local, 2), depth % 4)
        at = CHUNK * ((chunk - col) & 3) + BLK * (local & 3)
        at = jnp.where((local >= 0) & (local < 16), at, 4 * LANES)
        tiny = lax.broadcasted_iota(jnp.int32, codes.shape, 2) < HERE
        mixed_ref[start * USLOTS : (start + count) * USLOTS] = jnp.where(tiny, at, codes).reshape(-1, LANES)
    copy = pltpu.make_async_copy(mixed_ref, codes_ref, sem)
    copy.start()
    lane = lax.broadcasted_iota(jnp.int32, (8, LANES), 1)
    blank = jnp.zeros((8, LANES), jnp.float32)
    copy.wait()

    def fill(n, carry):
        j = (n // GROUP) % 4
        row = 2 * ((side + jnp.where(j == 1, 3, j - j // 2)) % 4) + lax.bitwise_xor(core, n // 32)
        place_in = n % GROUP
        panel = lax.bitwise_xor(depth // 4, place_in // 4) * 4 + ((depth - place_in) & 3)
        base = panel * PANEL + row * HERE
        blocks = [right_ref[n, u].astype(jnp.float32) for u in range(USLOTS)]
        for k in range(HERE):
            z = [[blank] * 3 for _ in range(3)]
            for u in range(USLOTS):
                at = codes_ref[n * USLOTS + u, k]
                rolled = pltpu.roll(blocks[u], (at + 4 * LANES - BLK * k) % LANES, 1)
                for q in range(3):
                    here = (lane + (q * LANES - at)).astype(jnp.uint32) < BLK
                    for v in range(3):
                        z[q][v] = jnp.where(here, rolled[8 * v : 8 * v + 8], z[q][v])
            for q in range(3):
                wide_ref[base + k, q] = jnp.concatenate(z[q] + [blank], axis=0).astype(jnp.bfloat16)
        return carry

    lax.fori_loop(0, 8 * GROUP, fill, 0, unroll=4)
    table_ref[...] = mixed_ref[0 : GROUP * USLOTS]


def fill(meta, rights):
    vmem = pl.BlockSpec(memory_space=pltpu.VMEM)
    lines = 8 * GROUP * USLOTS
    return pl.pallas_call(
        fill_kernel,
        out_shape=(
            jax.ShapeDtypeStruct((GROUP * PANEL, 3, KROW, LANES), jnp.bfloat16),
            jax.ShapeDtypeStruct((GROUP * USLOTS, LANES), jnp.int32),
        ),
        in_specs=[pl.BlockSpec(memory_space=pltpu.SMEM)] + [vmem] * len(rights),
        out_specs=(vmem, vmem),
        scratch_shapes=[
            pltpu.VMEM((8 * GROUP, USLOTS, APAD, LANES), jnp.bfloat16),
            pltpu.VMEM((lines, LANES), jnp.int32),
            pltpu.SMEM((lines, LANES), jnp.int32),
            pltpu.SemaphoreType.DMA,
        ],
        compiler_params=pltpu.CompilerParams(vmem_limit_bytes=16 * 1024 * 1024),
        cost_estimate=pl.CostEstimate(flops=3_000_000_000, bytes_accessed=8_000_000, transcendentals=0),
    )(meta, *rights)


def product_kernel(meta_ref, table_ref, wide_ref, *refs):
    lefts, outs, (far_ref, sum_ref, part_ref) = refs[:9], refs[9:16], refs[16:]
    depth = meta_ref[0]
    panels = [(depth + o) % GROUP for o in OFFSETS]
    lines = [(lax.bitwise_xor(p // 4, depth // 4) * 4 + ((depth - p) & 3)) * USLOTS for p in panels]
    half = ROWS // 2
    far_ref[:half] = lefts[7][...]
    far_ref[half:] = lefts[8][...]
    lefts = (*lefts[:7], far_ref)

    def step(g, carry):
        for m in range(8):
            i = g * 8 + m
            at = [
                p * PANEL + table_ref[line + s // 2, 16 + ROWS * (s % 2) + i]
                for p, line in zip(panels, lines)
                for s in range(SLOTS)
            ]
            weights = jnp.concatenate(
                [jnp.concatenate([wide_ref[n, q] for n in at], axis=0) for q in range(3)], axis=1
            )
            rows = jnp.concatenate([x[i] for x in lefts], axis=1)
            part_ref[m * BLK : m * BLK + APAD, :] = jnp.dot(rows, weights, preferred_element_type=jnp.float32)
        sum_ref[pl.ds(pl.multiple_of(g * 8 * BLK, 8), 8 * BLK), :] = part_ref[0 : 8 * BLK, :]
        return carry

    lax.fori_loop(0, ROWS // 8, step, 0)
    for q in range(3):
        turned = sum_ref[0:1152, q * LANES : (q + 1) * LANES].T[:, : ROWS * BLK]
        for ref, (first, last) in zip(outs, SPANS):
            low, high = max(first, q * LANES), min(last, (q + 1) * LANES)
            if low < high:
                ref[low - first : high - first, :] = turned[low - q * LANES : high - q * LANES]


def product(meta, table, wide, lefts):
    vmem = pl.BlockSpec(memory_space=pltpu.VMEM)
    smem = pl.BlockSpec(memory_space=pltpu.SMEM)
    return pl.pallas_call(
        product_kernel,
        out_shape=tuple(jax.ShapeDtypeStruct((b - a, ROWS * BLK), jnp.float32) for a, b in SPANS),
        in_specs=[smem, smem, vmem] + [vmem] * len(lefts),
        out_specs=(vmem,) * len(SPANS),
        scratch_shapes=[
            pltpu.VMEM((ROWS, APAD, LANES), jnp.bfloat16),
            pltpu.VMEM((1152, WIDE), jnp.float32),
            pltpu.VMEM((8 * APAD, WIDE), jnp.float32),
        ],
        compiler_params=pltpu.CompilerParams(vmem_limit_bytes=12 * 1024 * 1024),
        cost_estimate=pl.CostEstimate(flops=6_000_000_000, bytes_accessed=8_000_000, transcendentals=0),
    )(meta, table, wide, *lefts)


def shift(x, axis, by, n):
    return lax.ppermute(x, axis, [(i, (i + by) % n) for i in range(n)])


def body(left_values, left_columns, right_values, right_columns):
    c, d = lax.axis_index("col"), lax.axis_index("depth")
    meta = jnp.stack([d, lax.axis_index("row") % 2, lax.axis_index("row") // 2, c])
    tiles = pack_right(meta, right_values, right_columns, left_columns)
    left = pack_left(left_values)
    near = [tiles[0]] + [
        lax.ppermute(tiles[k], "depth", [(z, z // 4 * 4 + (z + k) % 4) for z in range(8)]) for k in (1, 2, 3)
    ]
    up1, down1 = shift(left, "depth", 1, 8), shift(left, "depth", -1, 8)
    half = jnp.stack(near, axis=0)
    other = shift(half, "depth", 4, 8)
    up1, down1, half, other = lax.optimization_barrier((up1, down1, half, other))
    right = jnp.concatenate([half, other], axis=0)
    f1, b1 = shift(right, "row", 2, 8), shift(right, "row", -2, 8)
    up2, down2 = shift(up1, "depth", 1, 8), shift(down1, "depth", -1, 8)
    up2, down2, f1, b1 = lax.optimization_barrier((up2, down2, f1, b1))
    swap = [(i, i ^ 1) for i in range(8)]
    f2, b2 = shift(f1[:4], "row", 2, 8), shift(b1[4:], "row", -2, 8)
    up3, down3 = shift(up2, "depth", 1, 8), shift(down2, "depth", -1, 8)
    others = [lax.ppermute(x, "row", swap) for x in (right, f1, b1)]
    up3, down3, f2, b2 = lax.optimization_barrier((up3, down3, f2, b2))
    others += [lax.ppermute(x, "row", swap) for x in (f2, b2)]
    edge = ROWS // 2
    up4, down4 = shift(up3[:edge], "depth", 1, 8), shift(down3[edge:], "depth", -1, 8)
    lefts = [left, up1, down1, up2, down2, up3, down3, up4, down4]
    wide, table = fill(meta, [right, f1, b1, f2, b2] + others)
    own, ahead_low, ahead_high, far_low, far_high, behind_low, behind_high = product(meta, table, wide, lefts)
    far_low = shift(far_low, "col", 1, 4)
    far_high = shift(far_high, "col", -1, 4)
    ahead_high = shift(ahead_high, "col", 1, 4)
    behind_low = shift(behind_low, "col", -1, 4)
    ahead_low = shift(ahead_low + far_low, "col", 1, 4)
    behind_high = shift(behind_high + far_high, "col", -1, 4)
    low = own[:48] + behind_low + ahead_low
    high = own[48:] + ahead_high + behind_high
    done = jnp.concatenate([low.astype(jnp.bfloat16), high.astype(jnp.bfloat16)], axis=0)
    home = [(y * 8 + z, (z % 4) * 8 + (z // 4) * 4 + (y ^ (z % 4))) for y in range(4) for z in range(8)]
    return lax.ppermute(done, ("col", "depth"), home).T


def solution(mesh):
    placed = (
        P("row", ("col", "depth"), None, None),
        P("row", ("col", "depth"), None),
        P(("col", "depth"), "row", None, None, None),
        P(("col", "depth"), "row", None, None),
    )
    return jax.shard_map(
        body, mesh=mesh, in_specs=placed, out_specs=P("row", ("col", "depth")), check_vma=False
    )
```

```python
import jax
import jax.numpy as jnp
from jax import lax
from jax.experimental import pallas as pl
from jax.experimental.pallas import tpu as pltpu
from jax.sharding import PartitionSpec as P


BLK = 23
LANES = 128
APAD = 24
KROW = 32
SLOTS = 4
USLOTS = 3
TILES = 4
PANEL = 40
HERE = 5
GROUP = 8
CHUNK = 96
WIDE = 4 * CHUNK
ROWS = 48
SPANS = ((0, 92), (96, 144), (144, 188), (192, 240), (240, 284), (288, 336), (336, 380))
STARTS = (0, 8, 16, 24, 28, 32, 40, 48, 56, 60)
OFFSETS = (0, 7, 1, 6, 2, 5, 3, 4)


def place(z, windows, lane, src, dst):
    first, last = src // LANES, (src + BLK - 1) // LANES
    shift = (dst - src) % LANES
    split = dst + min(BLK, LANES * (first + 1) - src)
    rolled = pltpu.roll(windows(first), shift, 1) if shift else windows(first)
    z = jnp.where((lane >= dst) & (lane < split), rolled, z)
    if last != first:
        rolled = pltpu.roll(windows(last), shift, 1) if shift else windows(last)
        z = jnp.where((lane >= split) & (lane < dst + BLK), rolled, z)
    return z


def pack_left_kernel(left_ref, out_ref, flat_ref, tmp_ref):
    for i in range(ROWS):
        block = left_ref[i].astype(jnp.float32)
        for j in range(5):
            width = min(LANES, BLK * BLK - j * LANES)
            flat_ref[j, i * SLOTS : (i + 1) * SLOTS, 0:width] = block[:, j * LANES : j * LANES + width]
    lane = lax.broadcasted_iota(jnp.int32, (ROWS, LANES), 1)
    for a in range(BLK):
        z = jnp.zeros((ROWS, LANES), jnp.float32)
        for s in range(SLOTS):
            z = place(
                z,
                lambda j, s=s: flat_ref[j, pl.ds(s, ROWS, stride=SLOTS), :],
                lane,
                BLK * a,
                KROW * s,
            )
        tmp_ref[pl.ds(a, ROWS, stride=APAD), :] = z
    tmp_ref[pl.ds(BLK, ROWS, stride=APAD), :] = jnp.zeros((ROWS, LANES), jnp.float32)
    for i in range(ROWS):
        out_ref[i] = tmp_ref[i * APAD : (i + 1) * APAD, :].astype(jnp.bfloat16)


def pack_left(left_values):
    vmem = pl.BlockSpec(memory_space=pltpu.VMEM)
    return pl.pallas_call(
        pack_left_kernel,
        out_shape=jax.ShapeDtypeStruct((ROWS, APAD, LANES), jnp.bfloat16),
        in_specs=[vmem],
        out_specs=vmem,
        scratch_shapes=[
            pltpu.VMEM((5, ROWS * SLOTS, LANES), jnp.float32),
            pltpu.VMEM((ROWS * APAD, LANES), jnp.float32),
        ],
        compiler_params=pltpu.CompilerParams(vmem_limit_bytes=8 * 1024 * 1024),
    )(left_values[:, 0])


def pack_right_kernel(meta_ref, right_ref, right_cols_ref, left_cols_ref, *refs):
    outs, (flat_ref, code_ref, tmp_ref) = refs[:TILES], refs[TILES:]
    for k in range(HERE):
        for u in range(USLOTS):
            n = (k * USLOTS + u) * 8
            flat_ref[n : n + TILES, 0 : BLK * BLK] = right_ref[k, u].astype(jnp.float32)
    code_ref[...] = jnp.zeros((8, LANES), jnp.float32)
    code_ref[0:SLOTS, 0:ROWS] = left_cols_ref[...].astype(jnp.float32)
    codes = code_ref[...]
    lane = lax.broadcasted_iota(jnp.int32, (8, LANES), 1)
    for u in range(USLOTS):
        for a in range(BLK):
            z = jnp.zeros((8, LANES), jnp.float32)
            for k in range(HERE):
                n = (k * USLOTS + u) * 8
                z = place(
                    z,
                    lambda j, n=n: flat_ref[n : n + 8, j * LANES : (j + 1) * LANES],
                    lane,
                    BLK * a,
                    BLK * k,
                )
            tmp_ref[u, pl.ds(a, 8, stride=APAD), :] = z
        code_ref[...] = jnp.zeros((8, LANES), jnp.float32)
        code_ref[0:TILES, 0:HERE] = right_cols_ref[u].astype(jnp.float32)
        z = code_ref[...]
        if u < 2:
            for h in range(2):
                line = codes[2 * u + h : 2 * u + h + 1, :]
                z = z + pltpu.roll(jnp.broadcast_to(line, (8, LANES)), 16 + ROWS * h, 1)
        tmp_ref[u, pl.ds(BLK, 8, stride=APAD), :] = z
    for t in range(TILES):
        tile = (meta_ref[0] + t) % TILES
        for u in range(USLOTS):
            rows = tmp_ref[u, pl.ds(pl.multiple_of(tile * APAD, 8), APAD), :]
            outs[t][u] = rows.astype(jnp.bfloat16)


def pack_right(meta, right_values, right_columns, left_columns):
    vmem = pl.BlockSpec(memory_space=pltpu.VMEM)
    return pl.pallas_call(
        pack_right_kernel,
        out_shape=(jax.ShapeDtypeStruct((USLOTS, APAD, LANES), jnp.bfloat16),) * TILES,
        in_specs=[pl.BlockSpec(memory_space=pltpu.SMEM)] + [vmem] * 3,
        out_specs=(vmem,) * TILES,
        scratch_shapes=[
            pltpu.VMEM((HERE * USLOTS * 8, 5 * LANES), jnp.float32),
            pltpu.VMEM((8, LANES), jnp.float32),
            pltpu.VMEM((USLOTS, 8 * APAD, LANES), jnp.float32),
        ],
        compiler_params=pltpu.CompilerParams(vmem_limit_bytes=8 * 1024 * 1024),
    )(
        meta,
        jnp.transpose(right_values[0], (0, 2, 1, 3)),
        jnp.transpose(right_columns[0], (2, 1, 0)),
        jnp.transpose(left_columns[:, 0], (1, 0)),
    )


def fill_kernel(meta_ref, *refs):
    rights, (wide_ref, table_ref) = refs[:-7], refs[-7:-5]
    right_ref, mixed_ref, turned_ref, codes_ref, sem = refs[-5:]
    depth, core, side, col = (meta_ref[m] for m in range(4))
    for source, piece in enumerate(rights):
        count = piece.shape[0]
        start = STARTS[source]
        right_ref[start : start + count] = piece[...]
        for n in range(count):
            for u in range(USLOTS):
                row = (start + n) * USLOTS + u
                mixed_ref[row : row + 1, :] = piece[n, u, BLK : BLK + 1, :].astype(jnp.float32)
    codes = jnp.concatenate(
        [mixed_ref[h * LANES : (h + 1) * LANES, :].T[0:8, :] for h in range(2)], axis=1
    ).astype(jnp.int32)
    local = codes - 16 * lax.shift_right_arithmetic(depth, 2)
    chunk = lax.bitwise_xor(lax.shift_right_arithmetic(local, 2), depth & 3)
    at = CHUNK * ((chunk - col) & 3) + BLK * (local & 3)
    at = jnp.where((local >= 0) & (local < 16), at, 4 * LANES)
    turned_ref[0:8, :] = at
    turned_ref[8:16, :] = (at + 4 * LANES - BLK * lax.broadcasted_iota(jnp.int32, at.shape, 0)) & (LANES - 1)
    copy = pltpu.make_async_copy(turned_ref, codes_ref, sem)
    copy.start()
    table_ref[...] = mixed_ref[0 : GROUP * USLOTS, :].astype(jnp.int32)
    lanes = [lax.broadcasted_iota(jnp.int32, (8, LANES), 1) + q * LANES for q in range(3)]
    blank = jnp.zeros((8, LANES), jnp.float32)
    copy.wait()

    def fill(n, carry):
        j = lax.shift_right_logical(n, 3) & 3
        x = side + jnp.where(j == 1, 3, j - lax.shift_right_logical(j, 1))
        row = 2 * (x & 3) + lax.bitwise_xor(core, lax.shift_right_logical(n, 5))
        spot = n & 7
        panel = lax.bitwise_xor(lax.shift_right_logical(depth, 2), lax.shift_right_logical(spot, 2)) * 4 + (
            (depth - spot) & 3
        )
        base = panel * PANEL + row * HERE
        first = n * USLOTS
        blocks = [right_ref[n, u].astype(jnp.float32) for u in range(USLOTS)]
        for k in range(HERE):
            z = [[blank] * 3 for _ in range(3)]
            for u in range(USLOTS):
                at = codes_ref[k, first + u]
                rolled = pltpu.roll(blocks[u], codes_ref[8 + k, first + u], 1)
                for q in range(3):
                    here = (lanes[q] - at).astype(jnp.uint32) < BLK
                    for v in range(3):
                        z[q][v] = jnp.where(here, rolled[8 * v : 8 * v + 8], z[q][v])
            for q in range(3):
                wide_ref[base + k, q] = jnp.concatenate(z[q] + [blank], axis=0).astype(jnp.bfloat16)
        return carry

    lax.fori_loop(0, 8 * GROUP, fill, 0, unroll=4)


def fill(meta, rights):
    vmem = pl.BlockSpec(memory_space=pltpu.VMEM)
    return pl.pallas_call(
        fill_kernel,
        out_shape=(
            jax.ShapeDtypeStruct((GROUP * PANEL, 3, KROW, LANES), jnp.bfloat16),
            jax.ShapeDtypeStruct((GROUP * USLOTS, LANES), jnp.int32),
        ),
        in_specs=[pl.BlockSpec(memory_space=pltpu.SMEM)] + [vmem] * len(rights),
        out_specs=(vmem, vmem),
        scratch_shapes=[
            pltpu.VMEM((8 * GROUP, USLOTS, APAD, LANES), jnp.bfloat16),
            pltpu.VMEM((2 * LANES, LANES), jnp.float32),
            pltpu.VMEM((16, 2 * LANES), jnp.int32),
            pltpu.SMEM((16, 2 * LANES), jnp.int32),
            pltpu.SemaphoreType.DMA,
        ],
        compiler_params=pltpu.CompilerParams(vmem_limit_bytes=16 * 1024 * 1024),
        cost_estimate=pl.CostEstimate(flops=3_000_000_000, bytes_accessed=8_000_000, transcendentals=0),
    )(meta, *rights)


def picked(meta_ref, table_ref, wide_ref, offsets, i):
    depth = meta_ref[0]
    at = []
    for o in offsets:
        panel = (depth + o) & 7
        line = lax.bitwise_xor(lax.shift_right_logical(panel, 2), lax.shift_right_logical(depth, 2)) * 4 + (
            (depth - panel) & 3
        )
        for s in range(SLOTS):
            at.append(panel * PANEL + table_ref[line * USLOTS + s // 2, 16 + ROWS * (s % 2) + i])
    return jnp.concatenate([jnp.concatenate([wide_ref[n, q] for n in at], axis=0) for q in range(3)], axis=1)


def early_kernel(meta_ref, table_ref, wide_ref, *refs):
    lefts, out_ref = refs[:4], refs[4]

    def step(g, carry):
        for m in range(8):
            i = g * 8 + m
            weights = picked(meta_ref, table_ref, wide_ref, OFFSETS[:4], i)
            rows = jnp.concatenate([x[i] for x in lefts], axis=1)
            out_ref[i] = jnp.dot(rows, weights, preferred_element_type=jnp.float32)
        return carry

    lax.fori_loop(0, ROWS // 8, step, 0)


def late_kernel(meta_ref, table_ref, wide_ref, early_ref, *refs):
    lefts, outs, (far_ref, sum_ref, part_ref) = refs[:5], refs[5:12], refs[12:]
    half = ROWS // 2
    far_ref[:half] = lefts[3][...]
    far_ref[half:] = lefts[4][...]
    lefts = (*lefts[:3], far_ref)

    def step(g, carry):
        for m in range(8):
            i = g * 8 + m
            weights = picked(meta_ref, table_ref, wide_ref, OFFSETS[4:], i)
            rows = jnp.concatenate([x[i] for x in lefts], axis=1)
            total = early_ref[i] + jnp.dot(rows, weights, preferred_element_type=jnp.float32)
            part_ref[m * BLK : m * BLK + APAD, :] = total
        sum_ref[pl.ds(pl.multiple_of(g * 8 * BLK, 8), 8 * BLK), :] = part_ref[0 : 8 * BLK, :]
        return carry

    lax.fori_loop(0, ROWS // 8, step, 0)
    for q in range(3):
        turned = sum_ref[0:1152, q * LANES : (q + 1) * LANES].T[:, : ROWS * BLK]
        for ref, (first, last) in zip(outs, SPANS):
            low, high = max(first, q * LANES), min(last, (q + 1) * LANES)
            if low < high:
                ref[low - first : high - first, :] = turned[low - q * LANES : high - q * LANES]


def product(meta, table, wide, lefts):
    vmem = pl.BlockSpec(memory_space=pltpu.VMEM)
    smem = pl.BlockSpec(memory_space=pltpu.SMEM)
    cost = pl.CostEstimate(flops=3_000_000_000, bytes_accessed=4_000_000, transcendentals=0)
    early = pl.pallas_call(
        early_kernel,
        out_shape=jax.ShapeDtypeStruct((ROWS, APAD, WIDE), jnp.float32),
        in_specs=[smem, smem, vmem] + [vmem] * 4,
        out_specs=vmem,
        compiler_params=pltpu.CompilerParams(vmem_limit_bytes=8 * 1024 * 1024),
        cost_estimate=cost,
    )(meta, table, wide, *lefts[:4])
    return pl.pallas_call(
        late_kernel,
        out_shape=tuple(jax.ShapeDtypeStruct((b - a, ROWS * BLK), jnp.float32) for a, b in SPANS),
        in_specs=[smem, smem, vmem, vmem] + [vmem] * 5,
        out_specs=(vmem,) * len(SPANS),
        scratch_shapes=[
            pltpu.VMEM((ROWS, APAD, LANES), jnp.bfloat16),
            pltpu.VMEM((1152, WIDE), jnp.float32),
            pltpu.VMEM((8 * APAD, WIDE), jnp.float32),
        ],
        compiler_params=pltpu.CompilerParams(vmem_limit_bytes=12 * 1024 * 1024),
        cost_estimate=cost,
    )(meta, table, wide, early, *lefts[4:])


def shift(x, axis, by, n):
    return lax.ppermute(x, axis, [(i, (i + by) % n) for i in range(n)])


def body(left_values, left_columns, right_values, right_columns):
    c, d = lax.axis_index("col"), lax.axis_index("depth")
    meta = jnp.stack([d, lax.axis_index("row") % 2, lax.axis_index("row") // 2, c])
    tiles = pack_right(meta, right_values, right_columns, left_columns)
    left = pack_left(left_values)
    near = [tiles[0]] + [
        lax.ppermute(tiles[k], "depth", [(z, z // 4 * 4 + (z + k) % 4) for z in range(8)]) for k in (1, 2, 3)
    ]
    up1, down1 = shift(left, "depth", 1, 8), shift(left, "depth", -1, 8)
    half = jnp.stack(near, axis=0)
    other = shift(half, "depth", 4, 8)
    right = jnp.concatenate([half, other], axis=0)
    swap = [(i, i ^ 1) for i in range(8)]
    f1, b1 = shift(right, "row", 2, 8), shift(right, "row", -2, 8)
    up2, down2 = shift(up1, "depth", 1, 8), shift(down1, "depth", -1, 8)
    f2, b2 = shift(f1[:4], "row", 2, 8), shift(b1[4:], "row", -2, 8)
    others = [lax.ppermute(x, "row", swap) for x in (right, f1, b1)]
    others += [lax.ppermute(x, "row", swap) for x in (f2, b2)]
    up3, down3 = shift(up2, "depth", 1, 8), shift(down2, "depth", -1, 8)
    edge = ROWS // 2
    up4, down4 = shift(up3[:edge], "depth", 1, 8), shift(down3[edge:], "depth", -1, 8)
    lefts = [left, up1, down1, up2, down2, up3, down3, up4, down4]
    wide, table = fill(meta, [right, f1, b1, f2, b2] + others)
    own, ahead_low, ahead_high, far_low, far_high, behind_low, behind_high = product(meta, table, wide, lefts)
    far_low = shift(far_low, "col", 1, 4)
    far_high = shift(far_high, "col", -1, 4)
    ahead_high = shift(ahead_high, "col", 1, 4)
    behind_low = shift(behind_low, "col", -1, 4)
    ahead_low = shift(ahead_low + far_low, "col", 1, 4)
    behind_high = shift(behind_high + far_high, "col", -1, 4)
    low = own[:48] + behind_low + ahead_low
    high = own[48:] + ahead_high + behind_high
    done = jnp.concatenate([low.astype(jnp.bfloat16), high.astype(jnp.bfloat16)], axis=0)
    home = [(y * 8 + z, (z % 4) * 8 + (z // 4) * 4 + (y ^ (z % 4))) for y in range(4) for z in range(8)]
    return lax.ppermute(done, ("col", "depth"), home).T


def solution(mesh):
    placed = (
        P("row", ("col", "depth"), None, None),
        P("row", ("col", "depth"), None),
        P(("col", "depth"), "row", None, None, None),
        P(("col", "depth"), "row", None, None),
    )
    return jax.shard_map(
        body, mesh=mesh, in_specs=placed, out_specs=P("row", ("col", "depth")), check_vma=False
    )
```

```python
import functools

import jax
import jax.numpy as jnp
from jax import lax
from jax.experimental import pallas as pl
from jax.experimental.pallas import tpu as pltpu
from jax.sharding import PartitionSpec as P


BLK = 23
LANES = 128
APAD = 24
KROW = 32
SLOTS = 4
USLOTS = 3
TILES = 4
PANEL = 40
HERE = 5
GROUP = 8
CHUNK = 96
WIDE = 4 * CHUNK
ROWS = 48
SPANS = ((0, 92), (96, 144), (144, 188), (192, 240), (240, 284), (288, 336), (336, 380))
STARTS = (0, 8, 16, 24, 28, 32, 40, 48, 56, 60)
OFFSETS = (0, 7, 1, 6, 2, 5, 3, 4)


def place(z, windows, lane, src, dst):
    first, last = src // LANES, (src + BLK - 1) // LANES
    shift = (dst - src) % LANES
    split = dst + min(BLK, LANES * (first + 1) - src)
    rolled = pltpu.roll(windows(first), shift, 1) if shift else windows(first)
    z = jnp.where((lane >= dst) & (lane < split), rolled, z)
    if last != first:
        rolled = pltpu.roll(windows(last), shift, 1) if shift else windows(last)
        z = jnp.where((lane >= split) & (lane < dst + BLK), rolled, z)
    return z


def pack_left_kernel(left_ref, out_ref, flat_ref, tmp_ref):
    for i in range(ROWS):
        block = left_ref[i].astype(jnp.float32)
        for j in range(5):
            width = min(LANES, BLK * BLK - j * LANES)
            flat_ref[j, i * SLOTS : (i + 1) * SLOTS, 0:width] = block[:, j * LANES : j * LANES + width]
    lane = lax.broadcasted_iota(jnp.int32, (ROWS, LANES), 1)
    for a in range(BLK):
        z = jnp.zeros((ROWS, LANES), jnp.float32)
        for s in range(SLOTS):
            z = place(
                z,
                lambda j, s=s: flat_ref[j, pl.ds(s, ROWS, stride=SLOTS), :],
                lane,
                BLK * a,
                KROW * s,
            )
        tmp_ref[pl.ds(a, ROWS, stride=APAD), :] = z
    tmp_ref[pl.ds(BLK, ROWS, stride=APAD), :] = jnp.zeros((ROWS, LANES), jnp.float32)
    for i in range(ROWS):
        out_ref[i] = tmp_ref[i * APAD : (i + 1) * APAD, :].astype(jnp.bfloat16)


def pack_left(left_values):
    vmem = pl.BlockSpec(memory_space=pltpu.VMEM)
    return pl.pallas_call(
        pack_left_kernel,
        out_shape=jax.ShapeDtypeStruct((ROWS, APAD, LANES), jnp.bfloat16),
        in_specs=[vmem],
        out_specs=vmem,
        scratch_shapes=[
            pltpu.VMEM((5, ROWS * SLOTS, LANES), jnp.float32),
            pltpu.VMEM((ROWS * APAD, LANES), jnp.float32),
        ],
        compiler_params=pltpu.CompilerParams(vmem_limit_bytes=8 * 1024 * 1024),
    )(left_values[:, 0])


def pack_right_kernel(meta_ref, right_in, right_cols_in, left_cols_in, *refs):
    outs, (flat_ref, code_ref, tmp_ref, right_ref, right_cols_ref, left_cols_ref, sems) = refs[:TILES], refs[TILES:]
    copies = [
        pltpu.make_async_copy(a, b, sems.at[n])
        for n, (a, b) in enumerate(
            ((right_in, right_ref), (right_cols_in, right_cols_ref), (left_cols_in, left_cols_ref))
        )
    ]
    for copy in copies:
        copy.start()
    for copy in copies:
        copy.wait()
    for k in range(HERE):
        for u in range(USLOTS):
            n = (k * USLOTS + u) * 8
            flat_ref[n : n + TILES, 0 : BLK * BLK] = right_ref[k, u].astype(jnp.float32)
    code_ref[...] = jnp.zeros((8, LANES), jnp.float32)
    code_ref[0:SLOTS, 0:ROWS] = left_cols_ref[...].astype(jnp.float32)
    codes = code_ref[...]
    lane = lax.broadcasted_iota(jnp.int32, (8, LANES), 1)
    for u in range(USLOTS):
        for a in range(BLK):
            z = jnp.zeros((8, LANES), jnp.float32)
            for k in range(HERE):
                n = (k * USLOTS + u) * 8
                z = place(
                    z,
                    lambda j, n=n: flat_ref[n : n + 8, j * LANES : (j + 1) * LANES],
                    lane,
                    BLK * a,
                    BLK * k,
                )
            tmp_ref[u, pl.ds(a, 8, stride=APAD), :] = z
        code_ref[...] = jnp.zeros((8, LANES), jnp.float32)
        code_ref[0:TILES, 0:HERE] = right_cols_ref[u].astype(jnp.float32)
        z = code_ref[...]
        if u < 2:
            for h in range(2):
                line = codes[2 * u + h : 2 * u + h + 1, :]
                z = z + pltpu.roll(jnp.broadcast_to(line, (8, LANES)), 16 + ROWS * h, 1)
        tmp_ref[u, pl.ds(BLK, 8, stride=APAD), :] = z
    for t in range(TILES):
        tile = lax.bitwise_xor((meta_ref[0] + t) & 3, 3 * lax.shift_right_logical(meta_ref[0], 2))
        for u in range(USLOTS):
            rows = tmp_ref[u, pl.ds(pl.multiple_of(tile * APAD, 8), APAD), :]
            outs[t][u] = rows.astype(jnp.bfloat16)


def pack_right(meta, right_values, right_columns, left_columns):
    vmem = pl.BlockSpec(memory_space=pltpu.VMEM)
    return pl.pallas_call(
        pack_right_kernel,
        out_shape=(jax.ShapeDtypeStruct((USLOTS, APAD, LANES), jnp.bfloat16),) * TILES,
        in_specs=[pl.BlockSpec(memory_space=pltpu.SMEM)] + [pl.BlockSpec(memory_space=pl.ANY)] * 3,
        out_specs=(vmem,) * TILES,
        scratch_shapes=[
            pltpu.VMEM((HERE * USLOTS * 8, 5 * LANES), jnp.float32),
            pltpu.VMEM((8, LANES), jnp.float32),
            pltpu.VMEM((USLOTS, 8 * APAD, LANES), jnp.float32),
            pltpu.VMEM((HERE, USLOTS, TILES, BLK * BLK), jnp.bfloat16),
            pltpu.VMEM((USLOTS, TILES, HERE), jnp.int32),
            pltpu.VMEM((SLOTS, ROWS), jnp.int32),
            pltpu.SemaphoreType.DMA((3,)),
        ],
    )(
        meta,
        jnp.transpose(right_values[0], (0, 2, 1, 3)),
        jnp.transpose(right_columns[0], (2, 1, 0)),
        jnp.transpose(left_columns[:, 0], (1, 0)),
    )


def fill_kernel(meta_ref, *refs):
    rights, (wide_ref, table_ref) = refs[:-7], refs[-7:-5]
    right_ref, mixed_ref, turned_ref, codes_ref, sem = refs[-5:]
    depth, core, side, col = (meta_ref[m] for m in range(4))
    for source, piece in enumerate(rights):
        count = piece.shape[0]
        start = STARTS[source]
        right_ref[start : start + count] = piece[...]
        for n in range(count):
            for u in range(USLOTS):
                row = (start + n) * USLOTS + u
                mixed_ref[row : row + 1, :] = piece[n, u, BLK : BLK + 1, :].astype(jnp.float32)
    codes = jnp.concatenate(
        [mixed_ref[h * LANES : (h + 1) * LANES, :].T[0:8, :] for h in range(2)], axis=1
    ).astype(jnp.int32)
    local = codes - 16 * lax.shift_right_logical(depth, 2)
    chunk = lax.bitwise_xor(lax.shift_right_arithmetic(local, 2), lax.bitwise_xor(depth, 7 * (depth >> 2)) & 3)
    at = CHUNK * ((chunk - col) & 3) + BLK * (local & 3)
    at = jnp.where((local >= 0) & (local < 16), at, 4 * LANES)
    turned_ref[0:8, :] = at
    turned_ref[8:16, :] = (at + 4 * LANES - BLK * lax.broadcasted_iota(jnp.int32, at.shape, 0)) & (LANES - 1)
    copy = pltpu.make_async_copy(turned_ref, codes_ref, sem)
    copy.start()
    table_ref[...] = mixed_ref[0 : GROUP * USLOTS, :].astype(jnp.int32)
    lanes = [lax.broadcasted_iota(jnp.int32, (8, LANES), 1) + q * LANES for q in range(3)]
    blank = jnp.zeros((8, LANES), jnp.float32)
    copy.wait()

    def fill(n, carry):
        j = lax.shift_right_logical(n, 3) & 3
        x = side + jnp.where(j == 1, 3, j - lax.shift_right_logical(j, 1))
        row = 2 * (x & 3) + lax.bitwise_xor(core, lax.shift_right_logical(n, 5))
        spot = n & 7
        other = lax.shift_right_logical(spot, 2)
        quad = lax.bitwise_xor(lax.shift_right_logical(depth, 2), other)
        panel = quad * 4 + ((lax.bitwise_xor(depth, 3 * other) - spot) & 3)
        base = panel * PANEL + row * HERE
        first = n * USLOTS
        blocks = [right_ref[n, u].astype(jnp.float32) for u in range(USLOTS)]
        for k in range(HERE):
            z = [[blank] * 3 for _ in range(3)]
            for u in range(USLOTS):
                at = codes_ref[k, first + u]
                rolled = pltpu.roll(blocks[u], codes_ref[8 + k, first + u], 1)
                for q in range(3):
                    here = (lanes[q] - at).astype(jnp.uint32) < BLK
                    for v in range(3):
                        z[q][v] = jnp.where(here, rolled[8 * v : 8 * v + 8], z[q][v])
            for q in range(3):
                wide_ref[base + k, q] = jnp.concatenate(z[q] + [blank], axis=0).astype(jnp.bfloat16)
        return carry

    lax.fori_loop(0, 8 * GROUP, fill, 0, unroll=4)


def fill(meta, rights):
    vmem = pl.BlockSpec(memory_space=pltpu.VMEM)
    return pl.pallas_call(
        fill_kernel,
        out_shape=(
            jax.ShapeDtypeStruct((GROUP * PANEL, 3, KROW, LANES), jnp.bfloat16),
            jax.ShapeDtypeStruct((GROUP * USLOTS, LANES), jnp.int32),
        ),
        in_specs=[pl.BlockSpec(memory_space=pltpu.SMEM)] + [vmem] * len(rights),
        out_specs=(vmem, vmem),
        scratch_shapes=[
            pltpu.VMEM((8 * GROUP, USLOTS, APAD, LANES), jnp.bfloat16),
            pltpu.VMEM((2 * LANES, LANES), jnp.float32),
            pltpu.VMEM((16, 2 * LANES), jnp.int32),
            pltpu.SMEM((16, 2 * LANES), jnp.int32),
            pltpu.SemaphoreType.DMA,
        ],
        compiler_params=pltpu.CompilerParams(vmem_limit_bytes=16 * 1024 * 1024),
        cost_estimate=pl.CostEstimate(flops=3_000_000_000, bytes_accessed=8_000_000, transcendentals=0),
    )(meta, *rights)


def picked(meta_ref, table_ref, wide_ref, offsets, i):
    depth = meta_ref[0]
    at = []
    for o in offsets:
        panel = (depth + o) & 7
        other = lax.shift_right_logical(lax.bitwise_xor(panel, depth), 2)
        line = other * 4 + ((lax.bitwise_xor(depth, 3 * other) - panel) & 3)
        for s in range(SLOTS):
            at.append(panel * PANEL + table_ref[line * USLOTS + s // 2, 16 + ROWS * (s % 2) + i])
    return jnp.concatenate([jnp.concatenate([wide_ref[n, q] for n in at], axis=0) for q in range(3)], axis=1)


def product_kernel(start, count, meta_ref, table_ref, wide_ref, *refs):
    lefts, outs, (sum_ref, part_ref) = refs[:9], refs[9:16], refs[16:]

    def steps(first, last, far_ref, skip):
        def step(g, carry):
            for m in range(8):
                i = g * 8 + m
                weights = picked(meta_ref, table_ref, wide_ref, OFFSETS, i)
                rows = jnp.concatenate([x[i] for x in lefts[:7]] + [far_ref[i - skip]], axis=1)
                part_ref[m * BLK : m * BLK + APAD, :] = jnp.dot(rows, weights, preferred_element_type=jnp.float32)
            at = pl.multiple_of((g - start) * 8 * BLK, 8)
            sum_ref[pl.ds(at, 8 * BLK), :] = part_ref[0 : 8 * BLK, :]
            return carry

        lax.fori_loop(first, last, step, 0)

    if start < 3:
        steps(start, min(3, start + count), lefts[7], 0)
    if start + count > 3:
        steps(max(3, start), start + count, lefts[8], ROWS // 2)
    width = count * 8 * BLK
    for q in range(3):
        turned = sum_ref[:, q * LANES : (q + 1) * LANES].T[:, :width]
        for ref, (first, last) in zip(outs, SPANS):
            low, high = max(first, q * LANES), min(last, (q + 1) * LANES)
            if low < high:
                ref[low - first : high - first, :] = turned[low - q * LANES : high - q * LANES]


def product(meta, table, wide, lefts, start, count):
    vmem = pl.BlockSpec(memory_space=pltpu.VMEM)
    smem = pl.BlockSpec(memory_space=pltpu.SMEM)
    width = count * 8 * BLK
    return pl.pallas_call(
        functools.partial(product_kernel, start, count),
        out_shape=tuple(jax.ShapeDtypeStruct((b - a, width), jnp.float32) for a, b in SPANS),
        in_specs=[smem, smem, vmem] + [vmem] * len(lefts),
        out_specs=(vmem,) * len(SPANS),
        scratch_shapes=[
            pltpu.VMEM((-(-width // LANES) * LANES, WIDE), jnp.float32),
            pltpu.VMEM((8 * APAD, WIDE), jnp.float32),
        ],
        compiler_params=pltpu.CompilerParams(vmem_limit_bytes=8 * 1024 * 1024),
        cost_estimate=pl.CostEstimate(flops=count * 1_000_000_000, bytes_accessed=8_000_000, transcendentals=0),
    )(meta, table, wide, *lefts)


def summed(parts):
    own, ahead_low, ahead_high, far_low, far_high, behind_low, behind_high = parts
    far_low = shift(far_low, "col", 1, 4)
    far_high = shift(far_high, "col", -1, 4)
    ahead_high = shift(ahead_high, "col", 1, 4)
    behind_low = shift(behind_low, "col", -1, 4)
    ahead_low = shift(ahead_low + far_low, "col", 1, 4)
    behind_high = shift(behind_high + far_high, "col", -1, 4)
    low = own[:48] + behind_low + ahead_low
    high = own[48:] + ahead_high + behind_high
    done = jnp.concatenate([low.astype(jnp.bfloat16), high.astype(jnp.bfloat16)], axis=0)
    home = []
    for y in range(4):
        for z in range(8):
            tile = min(z, 7 - z)
            home.append((y * 8 + z, tile * 8 + z // 4 * 4 + (y ^ tile)))
    return lax.ppermute(done, ("col", "depth"), home)


def shift(x, axis, by, n):
    return lax.ppermute(x, axis, [(i, (i + by) % n) for i in range(n)])


def body(left_values, left_columns, right_values, right_columns):
    c, d = lax.axis_index("col"), lax.axis_index("depth")
    meta = jnp.stack([d, lax.axis_index("row") % 2, lax.axis_index("row") // 2, c])
    tiles = pack_right(meta, right_values, right_columns, left_columns)
    left = pack_left(left_values)
    near = [tiles[0]] + [
        lax.ppermute(tiles[k], "depth", [(z, z // 4 * 4 + (z + k) % 4) for z in range(8)]) for k in (1, 2, 3)
    ]
    up1, down1 = shift(left, "depth", 1, 8), shift(left, "depth", -1, 8)
    half = jnp.stack(near, axis=0)
    other = lax.ppermute(half, "depth", [(z, 7 - z) for z in range(8)])
    right = jnp.concatenate([half, other], axis=0)
    swap = [(i, i ^ 1) for i in range(8)]
    f1, b1 = shift(right, "row", 2, 8), shift(right, "row", -2, 8)
    up2, down2 = shift(up1, "depth", 1, 8), shift(down1, "depth", -1, 8)
    f2, b2 = shift(f1[:4], "row", 2, 8), shift(b1[4:], "row", -2, 8)
    others = [lax.ppermute(x, "row", swap) for x in (right, f1, b1)]
    others += [lax.ppermute(x, "row", swap) for x in (f2, b2)]
    up3, down3 = shift(up2, "depth", 1, 8), shift(down2, "depth", -1, 8)
    edge = ROWS // 2
    up4, down4 = shift(up3[:edge], "depth", 1, 8), shift(down3[edge:], "depth", -1, 8)
    lefts = [left, up1, down1, up2, down2, up3, down3, up4, down4]
    wide, table = fill(meta, [right, f1, b1, f2, b2] + others)
    first = product(meta, table, wide, lefts, 0, 4)
    second = product(meta, table, wide, lefts, 4, 2)
    done = [summed(first), summed(second)]
    return jnp.concatenate(done, axis=1).T


def solution(mesh):
    placed = (
        P("row", ("col", "depth"), None, None),
        P("row", ("col", "depth"), None),
        P(("col", "depth"), "row", None, None, None),
        P(("col", "depth"), "row", None, None),
    )
    return jax.shard_map(
        body, mesh=mesh, in_specs=placed, out_specs=P("row", ("col", "depth")), check_vma=False
    )
```

```python
import functools

import jax
import jax.numpy as jnp
from jax import lax
from jax.experimental import pallas as pl
from jax.experimental.pallas import tpu as pltpu
from jax.sharding import PartitionSpec as P


BLK = 23
LANES = 128
APAD = 24
KROW = 32
SLOTS = 4
USLOTS = 3
TILES = 4
PANEL = 40
HERE = 5
GROUP = 8
CHUNK = 96
WIDE = 4 * CHUNK
ROWS = 48
SPANS = ((0, 92), (96, 144), (144, 188), (192, 240), (240, 284), (288, 336), (336, 380))
STARTS = (0, 8, 16, 24, 32, 40, 48, 56)
OFFSETS = (0, 7, 1, 6, 2, 5, 3, 4)


def place(z, windows, lane, src, dst):
    first, last = src // LANES, (src + BLK - 1) // LANES
    shift = (dst - src) % LANES
    split = dst + min(BLK, LANES * (first + 1) - src)
    rolled = pltpu.roll(windows(first), shift, 1) if shift else windows(first)
    z = jnp.where((lane >= dst) & (lane < split), rolled, z)
    if last != first:
        rolled = pltpu.roll(windows(last), shift, 1) if shift else windows(last)
        z = jnp.where((lane >= split) & (lane < dst + BLK), rolled, z)
    return z


def pack_left_kernel(left_ref, out_ref, flat_ref, tmp_ref):
    for i in range(ROWS):
        block = left_ref[i].astype(jnp.float32)
        for j in range(5):
            width = min(LANES, BLK * BLK - j * LANES)
            flat_ref[j, i * SLOTS : (i + 1) * SLOTS, 0:width] = block[:, j * LANES : j * LANES + width]
    lane = lax.broadcasted_iota(jnp.int32, (ROWS, LANES), 1)
    for a in range(BLK):
        z = jnp.zeros((ROWS, LANES), jnp.float32)
        for s in range(SLOTS):
            z = place(
                z,
                lambda j, s=s: flat_ref[j, pl.ds(s, ROWS, stride=SLOTS), :],
                lane,
                BLK * a,
                KROW * s,
            )
        tmp_ref[pl.ds(a, ROWS, stride=APAD), :] = z
    tmp_ref[pl.ds(BLK, ROWS, stride=APAD), :] = jnp.zeros((ROWS, LANES), jnp.float32)
    for i in range(ROWS):
        out_ref[i] = tmp_ref[i * APAD : (i + 1) * APAD, :].astype(jnp.bfloat16)


def pack_left(left_values):
    vmem = pl.BlockSpec(memory_space=pltpu.VMEM)
    return pl.pallas_call(
        pack_left_kernel,
        out_shape=jax.ShapeDtypeStruct((ROWS, APAD, LANES), jnp.bfloat16),
        in_specs=[vmem],
        out_specs=vmem,
        scratch_shapes=[
            pltpu.VMEM((5, ROWS * SLOTS, LANES), jnp.float32),
            pltpu.VMEM((ROWS * APAD, LANES), jnp.float32),
        ],
        compiler_params=pltpu.CompilerParams(vmem_limit_bytes=8 * 1024 * 1024),
    )(left_values[:, 0])


def pack_right_kernel(right_in, right_cols_in, left_cols_in, *refs):
    outs, (flat_ref, code_ref, tmp_ref, right_ref, right_cols_ref, left_cols_ref, sems) = refs[:1], refs[1:]
    copies = [
        pltpu.make_async_copy(a, b, sems.at[n])
        for n, (a, b) in enumerate(
            ((right_in, right_ref), (right_cols_in, right_cols_ref), (left_cols_in, left_cols_ref))
        )
    ]
    for copy in copies:
        copy.start()
    for copy in copies:
        copy.wait()
    for k in range(HERE):
        for u in range(USLOTS):
            n = (k * USLOTS + u) * 8
            flat_ref[n : n + TILES, 0 : BLK * BLK] = right_ref[k, u].astype(jnp.float32)
    code_ref[...] = jnp.zeros((8, LANES), jnp.float32)
    code_ref[0:SLOTS, 0:ROWS] = left_cols_ref[...].astype(jnp.float32)
    codes = code_ref[...]
    lane = lax.broadcasted_iota(jnp.int32, (8, LANES), 1)
    for u in range(USLOTS):
        for a in range(BLK):
            z = jnp.zeros((8, LANES), jnp.float32)
            for k in range(HERE):
                n = (k * USLOTS + u) * 8
                z = place(
                    z,
                    lambda j, n=n: flat_ref[n : n + 8, j * LANES : (j + 1) * LANES],
                    lane,
                    BLK * a,
                    BLK * k,
                )
            tmp_ref[u, pl.ds(a, 8, stride=APAD), :] = z
        code_ref[...] = jnp.zeros((8, LANES), jnp.float32)
        code_ref[0:TILES, 0:HERE] = right_cols_ref[u].astype(jnp.float32)
        z = code_ref[...]
        if u < 2:
            for h in range(2):
                line = codes[2 * u + h : 2 * u + h + 1, :]
                z = z + pltpu.roll(jnp.broadcast_to(line, (8, LANES)), 16 + ROWS * h, 1)
        tmp_ref[u, pl.ds(BLK, 8, stride=APAD), :] = z
    for d in range(GROUP):
        tile = min(d, 7 - d)
        for u in range(USLOTS):
            outs[0][d, u] = tmp_ref[u, tile * APAD : (tile + 1) * APAD, :].astype(jnp.bfloat16)


def pack_right(right_values, right_columns, left_columns):
    vmem = pl.BlockSpec(memory_space=pltpu.VMEM)
    return pl.pallas_call(
        pack_right_kernel,
        out_shape=jax.ShapeDtypeStruct((GROUP, USLOTS, APAD, LANES), jnp.bfloat16),
        in_specs=[pl.BlockSpec(memory_space=pl.ANY)] * 3,
        out_specs=vmem,
        scratch_shapes=[
            pltpu.VMEM((HERE * USLOTS * 8, 5 * LANES), jnp.float32),
            pltpu.VMEM((8, LANES), jnp.float32),
            pltpu.VMEM((USLOTS, 8 * APAD, LANES), jnp.float32),
            pltpu.VMEM((HERE, USLOTS, TILES, BLK * BLK), jnp.bfloat16),
            pltpu.VMEM((USLOTS, TILES, HERE), jnp.int32),
            pltpu.VMEM((SLOTS, ROWS), jnp.int32),
            pltpu.SemaphoreType.DMA((3,)),
        ],
    )(
        jnp.transpose(right_values[0], (0, 2, 1, 3)),
        jnp.transpose(right_columns[0], (2, 1, 0)),
        jnp.transpose(left_columns[:, 0], (1, 0)),
    )


def fill_kernel(meta_ref, *refs):
    rights, (wide_ref, table_ref) = refs[:-7], refs[-7:-5]
    right_ref, mixed_ref, turned_ref, codes_ref, sem = refs[-5:]
    depth, core, side, col = (meta_ref[m] for m in range(4))
    for source, piece in enumerate(rights):
        count = piece.shape[0]
        start = STARTS[source]
        right_ref[start : start + count] = piece[...]
        for n in range(count):
            for u in range(USLOTS):
                row = (start + n) * USLOTS + u
                mixed_ref[row : row + 1, :] = piece[n, u, BLK : BLK + 1, :].astype(jnp.float32)
    codes = jnp.concatenate(
        [mixed_ref[h * LANES : (h + 1) * LANES, :].T[0:8, :] for h in range(2)], axis=1
    ).astype(jnp.int32)
    local = codes - 16 * lax.shift_right_logical(depth, 2)
    chunk = lax.bitwise_xor(lax.shift_right_arithmetic(local, 2), lax.bitwise_xor(depth, 7 * (depth >> 2)) & 3)
    at = CHUNK * (((chunk - col) * (1 - 2 * core)) & 3) + BLK * (local & 3)
    at = jnp.where((local >= 0) & (local < 16), at, 4 * LANES)
    turned_ref[0:8, :] = at
    turned_ref[8:16, :] = (at + 4 * LANES - BLK * lax.broadcasted_iota(jnp.int32, at.shape, 0)) & (LANES - 1)
    copy = pltpu.make_async_copy(turned_ref, codes_ref, sem)
    copy.start()
    table_ref[...] = mixed_ref[0 : GROUP * USLOTS, :].astype(jnp.int32)
    lanes = [lax.broadcasted_iota(jnp.int32, (8, LANES), 1) + q * LANES for q in range(3)]
    blank = jnp.zeros((8, LANES), jnp.float32)
    copy.wait()

    def fill(n, carry):
        j = lax.shift_right_logical(n, 3) & 3
        owner = lax.bitwise_xor(core, lax.shift_right_logical(n, 5))
        x = side + (1 - 2 * owner) * jnp.where(j == 1, 3, j - lax.shift_right_logical(j, 1))
        row = 2 * (x & 3) + owner
        spot = n & 7
        base = spot * PANEL + row * HERE
        first = n * USLOTS
        blocks = [right_ref[n, u].astype(jnp.float32) for u in range(USLOTS)]
        for k in range(HERE):
            z = [[blank] * 3 for _ in range(3)]
            for u in range(USLOTS):
                at = codes_ref[k, first + u]
                rolled = pltpu.roll(blocks[u], codes_ref[8 + k, first + u], 1)
                for q in range(3):
                    here = (lanes[q] - at).astype(jnp.uint32) < BLK
                    for v in range(3):
                        z[q][v] = jnp.where(here, rolled[8 * v : 8 * v + 8], z[q][v])
            for q in range(3):
                wide_ref[base + k, q] = jnp.concatenate(z[q] + [blank], axis=0).astype(jnp.bfloat16)
        return carry

    lax.fori_loop(0, 8 * GROUP, fill, 0, unroll=4)


def fill(meta, rights):
    vmem = pl.BlockSpec(memory_space=pltpu.VMEM)
    return pl.pallas_call(
        fill_kernel,
        out_shape=(
            jax.ShapeDtypeStruct((GROUP * PANEL, 3, KROW, LANES), jnp.bfloat16),
            jax.ShapeDtypeStruct((GROUP * USLOTS, LANES), jnp.int32),
        ),
        in_specs=[pl.BlockSpec(memory_space=pltpu.SMEM)] + [vmem] * len(rights),
        out_specs=(vmem, vmem),
        scratch_shapes=[
            pltpu.VMEM((8 * GROUP, USLOTS, APAD, LANES), jnp.bfloat16),
            pltpu.VMEM((2 * LANES, LANES), jnp.float32),
            pltpu.VMEM((16, 2 * LANES), jnp.int32),
            pltpu.SMEM((16, 2 * LANES), jnp.int32),
            pltpu.SemaphoreType.DMA,
        ],
        compiler_params=pltpu.CompilerParams(vmem_limit_bytes=16 * 1024 * 1024),
        cost_estimate=pl.CostEstimate(flops=3_000_000_000, bytes_accessed=8_000_000, transcendentals=0),
    )(meta, *rights)


def picked(meta_ref, table_ref, wide_ref, offsets, i):
    depth = meta_ref[0]
    at = []
    for o in offsets:
        panel = (depth + o * (1 - 2 * meta_ref[1])) & 7
        line = panel
        for s in range(SLOTS):
            at.append(panel * PANEL + table_ref[line * USLOTS + s // 2, 16 + ROWS * (s % 2) + i])
    return jnp.concatenate([jnp.concatenate([wide_ref[n, q] for n in at], axis=0) for q in range(3)], axis=1)


def product_kernel(start, count, meta_ref, table_ref, wide_ref, *refs):
    lefts, outs, (sum_ref, part_ref) = refs[:9], refs[9:16], refs[16:]

    def steps(first, last, far_ref, skip):
        def step(g, carry):
            for m in range(8):
                i = g * 8 + m
                weights = picked(meta_ref, table_ref, wide_ref, OFFSETS, i)
                rows = jnp.concatenate([x[i] for x in lefts[:7]] + [far_ref[i - skip]], axis=1)
                part_ref[m * BLK : m * BLK + APAD, :] = jnp.dot(rows, weights, preferred_element_type=jnp.float32)
            at = pl.multiple_of((g - start) * 8 * BLK, 8)
            sum_ref[pl.ds(at, 8 * BLK), :] = part_ref[0 : 8 * BLK, :]
            return carry

        lax.fori_loop(first, last, step, 0)

    if start < 3:
        steps(start, min(3, start + count), lefts[7], 0)
    if start + count > 3:
        steps(max(3, start), start + count, lefts[8], ROWS // 2)
    width = count * 8 * BLK
    for q in range(3):
        turned = sum_ref[:, q * LANES : (q + 1) * LANES].T[:, :width]
        for ref, (first, last) in zip(outs, SPANS):
            low, high = max(first, q * LANES), min(last, (q + 1) * LANES)
            if low < high:
                ref[low - first : high - first, :] = turned[low - q * LANES : high - q * LANES]


def product(meta, table, wide, lefts, start, count):
    vmem = pl.BlockSpec(memory_space=pltpu.VMEM)
    smem = pl.BlockSpec(memory_space=pltpu.SMEM)
    width = count * 8 * BLK
    return pl.pallas_call(
        functools.partial(product_kernel, start, count),
        out_shape=tuple(jax.ShapeDtypeStruct((b - a, width), jnp.float32) for a, b in SPANS),
        in_specs=[smem, smem, vmem] + [vmem] * len(lefts),
        out_specs=(vmem,) * len(SPANS),
        scratch_shapes=[
            pltpu.VMEM((-(-width // LANES) * LANES, WIDE), jnp.float32),
            pltpu.VMEM((8 * APAD, WIDE), jnp.float32),
        ],
        compiler_params=pltpu.CompilerParams(vmem_limit_bytes=8 * 1024 * 1024),
        cost_estimate=pl.CostEstimate(flops=count * 1_000_000_000, bytes_accessed=8_000_000, transcendentals=0),
    )(meta, table, wide, *lefts)


def summed(parts):
    own, ahead_low, ahead_high, far_low, far_high, behind_low, behind_high = parts
    far_low = shift(far_low, "col", 1, 4)
    far_high = shift(far_high, "col", -1, 4)
    ahead_high = shift(ahead_high, "col", 1, 4)
    behind_low = shift(behind_low, "col", -1, 4)
    ahead_low = shift(ahead_low + far_low, "col", 1, 4)
    behind_high = shift(behind_high + far_high, "col", -1, 4)
    low = own[:48] + behind_low + ahead_low
    high = own[48:] + ahead_high + behind_high
    done = jnp.concatenate([low.astype(jnp.bfloat16), high.astype(jnp.bfloat16)], axis=0)
    home = []
    for y in range(4):
        for z in range(8):
            tile = min(z, 7 - z)
            home.append((y * 8 + z, tile * 8 + z // 4 * 4 + (y ^ tile)))
    return lax.ppermute(done, ("col", "depth"), home)


def shift(x, axis, by, n):
    pairs = []
    for r in range(8):
        way = by if r % 2 == 0 else -by
        if axis == "row":
            pairs.append((r, (r + way) % n))
        else:
            pairs += [(r * n + i, r * n + (i + way) % n) for i in range(n)]
    return lax.ppermute(x, axis if axis == "row" else ("row", axis), pairs)


def body(left_values, left_columns, right_values, right_columns):
    c, d = lax.axis_index("col"), lax.axis_index("depth")
    meta = jnp.stack([d, lax.axis_index("row") % 2, lax.axis_index("row") // 2, c])
    tiles = pack_right(right_values, right_columns, left_columns)
    left = pack_left(left_values)
    right = lax.all_to_all(tiles, "depth", 0, 0)
    up1, down1 = shift(left, "depth", 1, 8), shift(left, "depth", -1, 8)
    up1, down1, right = lax.optimization_barrier((up1, down1, right))
    swap = [(i, i ^ 1) for i in range(8)]
    f2 = shift(right, "row", 4, 8)
    f1, b1 = shift(right, "row", 2, 8), shift(right, "row", -2, 8)
    up2, down2 = shift(up1, "depth", 1, 8), shift(down1, "depth", -1, 8)
    others = [lax.ppermute(x, "row", swap) for x in (right, f1, b1)]
    others += [lax.ppermute(f2, "row", swap)]
    up3, down3 = shift(up2, "depth", 1, 8), shift(down2, "depth", -1, 8)
    edge = ROWS // 2
    up4, down4 = shift(up3[:edge], "depth", 1, 8), shift(down3[edge:], "depth", -1, 8)
    lefts = [left, up1, down1, up2, down2, up3, down3, up4, down4]
    wide, table = fill(meta, [right, f1, b1, f2] + others)
    parts = product(meta, table, wide, lefts, 0, 6)
    return summed(parts).T


def solution(mesh):
    placed = (
        P("row", ("col", "depth"), None, None),
        P("row", ("col", "depth"), None),
        P(("col", "depth"), "row", None, None, None),
        P(("col", "depth"), "row", None, None),
    )
    return jax.shard_map(
        body, mesh=mesh, in_specs=placed, out_specs=P("row", ("col", "depth")), check_vma=False
    )
```

```python
import functools

import jax
import jax.numpy as jnp
from jax import lax
from jax.experimental import pallas as pl
from jax.experimental.pallas import tpu as pltpu
from jax.sharding import PartitionSpec as P


BLK = 23
LANES = 128
APAD = 24
KROW = 32
SLOTS = 4
USLOTS = 3
TILES = 4
PANEL = 40
HERE = 5
GROUP = 8
CHUNK = 96
WIDE = 4 * CHUNK
ROWS = 48
SPANS = ((0, 92), (96, 144), (144, 188), (192, 240), (240, 284), (288, 336), (336, 380))
OFFSETS = (0, 7, 1, 6, 2, 5, 3, 4)


def place(z, windows, lane, src, dst):
    first, last = src // LANES, (src + BLK - 1) // LANES
    shift = (dst - src) % LANES
    split = dst + min(BLK, LANES * (first + 1) - src)
    rolled = pltpu.roll(windows(first), shift, 1) if shift else windows(first)
    z = jnp.where((lane >= dst) & (lane < split), rolled, z)
    if last != first:
        rolled = pltpu.roll(windows(last), shift, 1) if shift else windows(last)
        z = jnp.where((lane >= split) & (lane < dst + BLK), rolled, z)
    return z


def pack_left_kernel(left_ref, out_ref, flat_ref, tmp_ref):
    for i in range(ROWS):
        block = left_ref[i].astype(jnp.float32)
        for j in range(5):
            width = min(LANES, BLK * BLK - j * LANES)
            flat_ref[j, i * SLOTS : (i + 1) * SLOTS, 0:width] = block[:, j * LANES : j * LANES + width]
    lane = lax.broadcasted_iota(jnp.int32, (ROWS, LANES), 1)
    for a in range(BLK):
        z = jnp.zeros((ROWS, LANES), jnp.float32)
        for s in range(SLOTS):
            z = place(
                z,
                lambda j, s=s: flat_ref[j, pl.ds(s, ROWS, stride=SLOTS), :],
                lane,
                BLK * a,
                KROW * s,
            )
        tmp_ref[pl.ds(a, ROWS, stride=APAD), :] = z
    tmp_ref[pl.ds(BLK, ROWS, stride=APAD), :] = jnp.zeros((ROWS, LANES), jnp.float32)
    for i in range(ROWS):
        out_ref[i] = tmp_ref[i * APAD : (i + 1) * APAD, :].astype(jnp.bfloat16)


def pack_left(left_values):
    vmem = pl.BlockSpec(memory_space=pltpu.VMEM)
    return pl.pallas_call(
        pack_left_kernel,
        out_shape=jax.ShapeDtypeStruct((ROWS, APAD, LANES), jnp.bfloat16),
        in_specs=[vmem],
        out_specs=vmem,
        scratch_shapes=[
            pltpu.VMEM((5, ROWS * SLOTS, LANES), jnp.float32),
            pltpu.VMEM((ROWS * APAD, LANES), jnp.float32),
        ],
        compiler_params=pltpu.CompilerParams(vmem_limit_bytes=8 * 1024 * 1024),
    )(left_values[:, 0])


def pack_right_kernel(right_in, right_cols_in, left_cols_in, *refs):
    outs, (flat_ref, code_ref, tmp_ref, right_ref, right_cols_ref, left_cols_ref, sems) = refs[:1], refs[1:]
    copies = [
        pltpu.make_async_copy(a, b, sems.at[n])
        for n, (a, b) in enumerate(
            ((right_in, right_ref), (right_cols_in, right_cols_ref), (left_cols_in, left_cols_ref))
        )
    ]
    for copy in copies:
        copy.start()
    for copy in copies:
        copy.wait()
    for k in range(HERE):
        for u in range(USLOTS):
            n = (k * USLOTS + u) * 8
            flat_ref[n : n + TILES, 0 : BLK * BLK] = right_ref[k, u].astype(jnp.float32)
    code_ref[...] = jnp.zeros((8, LANES), jnp.float32)
    code_ref[0:SLOTS, 0:ROWS] = left_cols_ref[...].astype(jnp.float32)
    codes = code_ref[...]
    lane = lax.broadcasted_iota(jnp.int32, (8, LANES), 1)
    for u in range(USLOTS):
        for a in range(BLK):
            z = jnp.zeros((8, LANES), jnp.float32)
            for k in range(HERE):
                n = (k * USLOTS + u) * 8
                z = place(
                    z,
                    lambda j, n=n: flat_ref[n : n + 8, j * LANES : (j + 1) * LANES],
                    lane,
                    BLK * a,
                    BLK * k,
                )
            tmp_ref[u, pl.ds(a, 8, stride=APAD), :] = z
        code_ref[...] = jnp.zeros((8, LANES), jnp.float32)
        code_ref[0:TILES, 0:HERE] = right_cols_ref[u].astype(jnp.float32)
        z = code_ref[...]
        if u < 2:
            for h in range(2):
                line = codes[2 * u + h : 2 * u + h + 1, :]
                z = z + pltpu.roll(jnp.broadcast_to(line, (8, LANES)), 16 + ROWS * h, 1)
        tmp_ref[u, pl.ds(BLK, 8, stride=APAD), :] = z
    for d in range(GROUP):
        tile = min(d, 7 - d)
        for u in range(USLOTS):
            outs[0][d, u] = tmp_ref[u, tile * APAD : (tile + 1) * APAD, :].astype(jnp.bfloat16)


def pack_right(right_values, right_columns, left_columns):
    vmem = pl.BlockSpec(memory_space=pltpu.VMEM)
    return pl.pallas_call(
        pack_right_kernel,
        out_shape=jax.ShapeDtypeStruct((GROUP, USLOTS, APAD, LANES), jnp.bfloat16),
        in_specs=[pl.BlockSpec(memory_space=pl.ANY)] * 3,
        out_specs=vmem,
        scratch_shapes=[
            pltpu.VMEM((HERE * USLOTS * 8, 5 * LANES), jnp.float32),
            pltpu.VMEM((8, LANES), jnp.float32),
            pltpu.VMEM((USLOTS, 8 * APAD, LANES), jnp.float32),
            pltpu.VMEM((HERE, USLOTS, TILES, BLK * BLK), jnp.bfloat16),
            pltpu.VMEM((USLOTS, TILES, HERE), jnp.int32),
            pltpu.VMEM((SLOTS, ROWS), jnp.int32),
            pltpu.SemaphoreType.DMA((3,)),
        ],
    )(
        jnp.transpose(right_values[0], (0, 2, 1, 3)),
        jnp.transpose(right_columns[0], (2, 1, 0)),
        jnp.transpose(left_columns[:, 0], (1, 0)),
    )


def fill_kernel(theirs, meta_ref, *refs):
    rights, refs = refs[:4], refs[4 + theirs :]
    wide_ref, refs = refs[0], refs[1:]
    right_ref, mixed_ref, turned_ref, codes_ref, sem = refs[-5:]
    depth, core, side, col = (meta_ref[m] for m in range(4))
    owner = lax.bitwise_xor(core, theirs)
    for source, piece in enumerate(rights):
        count = piece.shape[0]
        start = source * GROUP
        right_ref[start : start + count] = piece[...]
        for n in range(count):
            for u in range(USLOTS):
                row = (start + n) * USLOTS + u
                mixed_ref[row : row + 1, :] = piece[n, u, BLK : BLK + 1, :].astype(jnp.float32)
    codes = mixed_ref[...].T[0:8, :].astype(jnp.int32)
    local = codes - 16 * lax.shift_right_logical(depth, 2)
    chunk = lax.bitwise_xor(lax.shift_right_arithmetic(local, 2), lax.bitwise_xor(depth, 7 * (depth >> 2)) & 3)
    at = CHUNK * (((chunk - col) * (1 - 2 * core)) & 3) + BLK * (local & 3)
    at = jnp.where((local >= 0) & (local < 16), at, 4 * LANES)
    turned_ref[0:8, :] = at
    turned_ref[8:16, :] = (at + 4 * LANES - BLK * lax.broadcasted_iota(jnp.int32, at.shape, 0)) & (LANES - 1)
    copy = pltpu.make_async_copy(turned_ref, codes_ref, sem)
    copy.start()
    if not theirs:
        refs[0][...] = mixed_ref[0 : GROUP * USLOTS, :].astype(jnp.int32)
    lanes = [lax.broadcasted_iota(jnp.int32, (8, LANES), 1) + q * LANES for q in range(3)]
    blank = jnp.zeros((8, LANES), jnp.float32)
    copy.wait()

    def fill(n, carry):
        j = lax.shift_right_logical(n, 3)
        x = side + (1 - 2 * owner) * jnp.where(j == 1, 3, j - lax.shift_right_logical(j, 1))
        row = 2 * (x & 3) + owner
        spot = n & 7
        base = spot * PANEL + row * HERE
        first = n * USLOTS
        blocks = [right_ref[n, u].astype(jnp.float32) for u in range(USLOTS)]
        for k in range(HERE):
            z = [[blank] * 3 for _ in range(3)]
            for u in range(USLOTS):
                at = codes_ref[k, first + u]
                rolled = pltpu.roll(blocks[u], codes_ref[8 + k, first + u], 1)
                for q in range(3):
                    here = (lanes[q] - at).astype(jnp.uint32) < BLK
                    for v in range(3):
                        z[q][v] = jnp.where(here, rolled[8 * v : 8 * v + 8], z[q][v])
            for q in range(3):
                wide_ref[base + k, q] = jnp.concatenate(z[q] + [blank], axis=0).astype(jnp.bfloat16)
        return carry

    lax.fori_loop(0, 4 * GROUP, fill, 0, unroll=8)


def fill(meta, rights, wide=None):
    vmem = pl.BlockSpec(memory_space=pltpu.VMEM)
    theirs = 0 if wide is None else 1
    shapes = (
        jax.ShapeDtypeStruct((GROUP * PANEL, 3, KROW, LANES), jnp.bfloat16),
        jax.ShapeDtypeStruct((GROUP * USLOTS, LANES), jnp.int32),
    )
    return pl.pallas_call(
        functools.partial(fill_kernel, theirs),
        out_shape=shapes[: 2 - theirs],
        in_specs=[pl.BlockSpec(memory_space=pltpu.SMEM)] + [vmem] * (4 + theirs),
        out_specs=(vmem, vmem)[: 2 - theirs],
        scratch_shapes=[
            pltpu.VMEM((4 * GROUP, USLOTS, APAD, LANES), jnp.bfloat16),
            pltpu.VMEM((LANES, LANES), jnp.float32),
            pltpu.VMEM((16, LANES), jnp.int32),
            pltpu.SMEM((16, LANES), jnp.int32),
            pltpu.SemaphoreType.DMA,
        ],
        input_output_aliases={5: 0} if theirs else {},
        compiler_params=pltpu.CompilerParams(vmem_limit_bytes=10 * 1024 * 1024),
        cost_estimate=pl.CostEstimate(flops=1_500_000_000, bytes_accessed=4_000_000, transcendentals=0),
    )(meta, *rights, *([wide] if theirs else []))


def picked(meta_ref, table_ref, wide_ref, offsets, i):
    depth = meta_ref[0]
    at = []
    for o in offsets:
        panel = (depth + o * (1 - 2 * meta_ref[1])) & 7
        line = panel
        for s in range(SLOTS):
            at.append(panel * PANEL + table_ref[line * USLOTS + s // 2, 16 + ROWS * (s % 2) + i])
    return jnp.concatenate([jnp.concatenate([wide_ref[n, q] for n in at], axis=0) for q in range(3)], axis=1)


def product_kernel(meta_ref, table_ref, wide_ref, *refs):
    lefts, outs, (sum_ref, part_ref) = refs[:GROUP], refs[GROUP : GROUP + 7], refs[GROUP + 7 :]

    def step(g, carry):
        for m in range(8):
            i = g * 8 + m
            weights = picked(meta_ref, table_ref, wide_ref, OFFSETS, i)
            rows = jnp.concatenate([x[i] for x in lefts], axis=1)
            part_ref[m * BLK : m * BLK + APAD, :] = jnp.dot(rows, weights, preferred_element_type=jnp.float32)
        sum_ref[pl.ds(pl.multiple_of(g * 8 * BLK, 8), 8 * BLK), :] = part_ref[0 : 8 * BLK, :]
        return carry

    lax.fori_loop(0, ROWS // 8, step, 0)
    for q in range(3):
        turned = sum_ref[:, q * LANES : (q + 1) * LANES].T[:, : ROWS * BLK]
        for ref, (first, last) in zip(outs, SPANS):
            low, high = max(first, q * LANES), min(last, (q + 1) * LANES)
            if low < high:
                ref[low - first : high - first, :] = turned[low - q * LANES : high - q * LANES]


def product(meta, table, wide, lefts):
    vmem = pl.BlockSpec(memory_space=pltpu.VMEM)
    smem = pl.BlockSpec(memory_space=pltpu.SMEM)
    return pl.pallas_call(
        product_kernel,
        out_shape=tuple(jax.ShapeDtypeStruct((b - a, ROWS * BLK), jnp.float32) for a, b in SPANS),
        in_specs=[smem, smem, vmem] + [vmem] * len(lefts),
        out_specs=(vmem,) * len(SPANS),
        scratch_shapes=[
            pltpu.VMEM((9 * LANES, WIDE), jnp.float32),
            pltpu.VMEM((8 * APAD, WIDE), jnp.float32),
        ],
        compiler_params=pltpu.CompilerParams(vmem_limit_bytes=8 * 1024 * 1024),
        cost_estimate=pl.CostEstimate(flops=6_000_000_000, bytes_accessed=8_000_000, transcendentals=0),
    )(meta, table, wide, *lefts)


def summed(parts):
    own, ahead_low, ahead_high, far_low, far_high, behind_low, behind_high = parts
    far_low = shift(far_low, "col", 1, 4)
    far_high = shift(far_high, "col", -1, 4)
    ahead_high = shift(ahead_high, "col", 1, 4)
    behind_low = shift(behind_low, "col", -1, 4)
    ahead_low = shift(ahead_low + far_low, "col", 1, 4)
    behind_high = shift(behind_high + far_high, "col", -1, 4)
    low = own[:48] + behind_low + ahead_low
    high = own[48:] + ahead_high + behind_high
    done = jnp.concatenate([low.astype(jnp.bfloat16), high.astype(jnp.bfloat16)], axis=0)
    home = []
    for y in range(4):
        for z in range(8):
            tile = min(z, 7 - z)
            home.append((y * 8 + z, tile * 8 + z // 4 * 4 + (y ^ tile)))
    return lax.ppermute(done, ("col", "depth"), home)


def shift(x, axis, by, n):
    pairs = []
    for r in range(8):
        way = by if r % 2 == 0 else -by
        if axis == "row":
            pairs.append((r, (r + way) % n))
        else:
            pairs += [(r * n + i, r * n + (i + way) % n) for i in range(n)]
    return lax.ppermute(x, axis if axis == "row" else ("row", axis), pairs)


def body(left_values, left_columns, right_values, right_columns):
    c, d = lax.axis_index("col"), lax.axis_index("depth")
    meta = jnp.stack([d, lax.axis_index("row") % 2, lax.axis_index("row") // 2, c])
    tiles = pack_right(right_values, right_columns, left_columns)
    left = pack_left(left_values)
    right = lax.all_to_all(tiles, "depth", 0, 0)
    up1, down1 = shift(left, "depth", 1, 8), shift(left, "depth", -1, 8)
    up1, down1, right = lax.optimization_barrier((up1, down1, right))
    swap = [(i, i ^ 1) for i in range(8)]
    f2 = shift(right, "row", 4, 8)
    f1, b1 = shift(right, "row", 2, 8), shift(right, "row", -2, 8)
    up2, down2 = shift(up1, "depth", 1, 8), shift(down1, "depth", -1, 8)
    others = [lax.ppermute(x, "row", swap) for x in (right, f1, b1)]
    others += [lax.ppermute(f2, "row", swap)]
    up3, down3 = shift(up2, "depth", 1, 8), shift(down2, "depth", -1, 8)
    up4 = shift(up3, "depth", 1, 8)
    lefts = [left, up1, down1, up2, down2, up3, down3, up4]
    wide, table = fill(meta, [right, f1, b1, f2])
    (wide,) = fill(meta, others, wide)
    parts = product(meta, table, wide, lefts)
    return summed(parts).T


def solution(mesh):
    placed = (
        P("row", ("col", "depth"), None, None),
        P("row", ("col", "depth"), None),
        P(("col", "depth"), "row", None, None, None),
        P(("col", "depth"), "row", None, None),
    )
    return jax.shard_map(
        body, mesh=mesh, in_specs=placed, out_specs=P("row", ("col", "depth")), check_vma=False
    )
```
